256 devices in a mesh: seq: 32 (over y, z), batch: 8 (over x, core).
Axes of the slice: x: 4, y: 4, z: 8, core: 2. Of those that a mesh axis runs over, the one named last changes fastest.
Arguments:
- conv_input: bfloat16 [32768, 8192], P(('batch', 'seq')), parts along dimension 0, may hold values from -6 to 6
- gate_input: bfloat16 [32768, 8192], P(('batch', 'seq')), parts along dimension 0, may hold values from -6 to 6
- conv_weight: bfloat16 [4, 8192], P(None, 'seq'), may hold values from -3 to 3
- conv_bias: bfloat16 [8192], P('seq'), may hold values from -3 to 3
- x_weight: bfloat16 [8192, 288], P('seq'), may hold values from -0.0625 to 0.0625
- dt_gain: float32 [256], replicated, may hold values from 0.5 to 1.5
- dt_weight: bfloat16 [256, 8192], P(None, 'seq'), may hold values from -0.375 to 0.375
- dt_bias: float32 [8192], P('seq'), may hold values from -6.9 to -2.3
- a_log: float32 [16, 8192], P(None, 'seq'), may hold values from 0 to 2.77
- skip: float32 [8192], P('seq'), may hold values from 0.5 to 1.5
Outputs:
- mixed: bfloat16 [32768, 8192], P(('batch', 'seq')), parts along dimension 0
The draws below stay inside these ranges and needn't reach their ends.
There are 8 independent parts, one for each index of `batch`. The reference program is written for one: setup_inputs(seed, part) draws one part's arguments, and reference() takes and returns one part's arrays. A program takes and returns all parts, laid end to end along the dimension named above; an argument that names none is the same for every part. Nothing has to cross between parts.
All inputs are finite; a program needn't handle non-finite values.
Results may differ from the reference program's by a relative error of at most 0.0085.
Values may be sent and summed in bfloat16 or wider, within the bound.
A program may use at most 128 MiB of HBM per device.

```python
import jax
import jax.numpy as jnp
from jax import lax

INNER = 8192
STATE = 16
DT_RANK = 256
CONV = 4
LENGTH = 4096
PROJ = 288


def block_scale(key, extent, pieces, low, top_value):
    def one(axis_at, blocks):
        steps = jax.random.uniform(jax.random.fold_in(jax.random.fold_in(key, 6), axis_at), (blocks,), jnp.float32, low / len(pieces), top_value / len(pieces))
        return jnp.repeat(jnp.exp(steps), extent[axis_at] // blocks).reshape((-1,) + (1,) * (len(extent) - axis_at - 1))

    loudness = one(*pieces[0])
    for cut in pieces[1:]:
        loudness = loudness * one(*cut)
    return loudness


def centred(stream_key, shape, scale, limit, shards=(), kind=jnp.bfloat16):
    drawn = scale * jax.random.normal(stream_key, shape, jnp.float32)
    if shards:
        drawn = drawn * block_scale(stream_key, shape, shards, -0.22, 0.18)
    return jnp.clip(drawn, -limit, limit).astype(kind)


def setup_inputs(seed: int = 0, part: int = 0) -> dict:
    key_list = jax.random.split(jax.random.key(seed), 11)
    part_splits = jax.random.split(jax.random.fold_in(key_list[10], part), 11)
    conv_input = centred(part_splits[0], (LENGTH, INNER), 1.0, 6.0, ((0, 32),))
    gate_input = centred(part_splits[1], (LENGTH, INNER), 1.0, 6.0, ((0, 32),))
    conv_weight = centred(key_list[2], (CONV, INNER), CONV ** -0.5, 3.0, ((1, 32),))
    conv_bias = centred(key_list[3], (INNER,), 0.5, 3.0, ((0, 32),))
    x_weight = centred(key_list[4], (INNER, PROJ), INNER ** -0.5, 0.0625, ((0, 32),))
    dt_gain = jnp.clip(1.0 + 0.1 * jax.random.normal(key_list[5], (DT_RANK,), jnp.float32), 0.5, 1.5)
    dt_weight = centred(key_list[6], (DT_RANK, INNER), DT_RANK ** -0.5, 0.375, ((1, 32),))
    dt_bias = jnp.clip(-6.9 + 4.6000001430511475 * jax.random.uniform(key_list[7], (INNER,), jnp.float32) ** block_scale(key_list[7], (INNER,), ((0, 32),), -0.2, 0.2), -6.9, -2.3)
    a_log = jnp.clip(2.77 * jax.random.uniform(key_list[8], (STATE, INNER), jnp.float32) ** block_scale(key_list[8], (STATE, INNER), ((1, 32),), -0.2, 0.2), 0.0, 2.77)
    skip = jnp.clip(1.0 + 0.1 * jax.random.normal(key_list[9], (INNER,), jnp.float32), 0.5, 1.5)
    return dict(conv_input=conv_input, gate_input=gate_input, conv_weight=conv_weight, conv_bias=conv_bias, x_weight=x_weight, dt_gain=dt_gain, dt_weight=dt_weight, dt_bias=dt_bias, a_log=a_log, skip=skip)


def convolve(inputs, weight, bias):
    rows = inputs.shape[0]
    width = weight.shape[0]
    padded = jnp.concatenate([jnp.zeros((width - 1, inputs.shape[1]), jnp.float32), inputs.astype(jnp.float32)], 0)
    total = bias.astype(jnp.float32)[None, :]
    for tap in range(width):
        total = total + weight[tap].astype(jnp.float32)[None, :] * padded[tap:tap + rows]
    return jax.nn.silu(total).astype(jnp.bfloat16)

def reference(conv_input, gate_input, conv_weight, conv_bias, x_weight, dt_gain, dt_weight, dt_bias, a_log, skip):
    xc = convolve(conv_input, conv_weight, conv_bias)
    proj = jnp.dot(xc, x_weight, preferred_element_type=jnp.float32)
    dt_low = proj[:, :DT_RANK]
    bmat = proj[:, DT_RANK:DT_RANK + STATE]
    cmat = proj[:, DT_RANK + STATE:]
    normed = (dt_low * lax.rsqrt(lax.optimization_barrier(jnp.mean(dt_low * dt_low, axis=1, keepdims=True)) + 1e-06) * dt_gain[None, :]).astype(jnp.bfloat16)
    step = jax.nn.softplus(jnp.dot(normed, dt_weight, preferred_element_type=jnp.float32) + dt_bias[None, :])
    rate = -jnp.exp(a_log)
    xfloat = xc.astype(jnp.float32)

    def advance(state, inputs):
        step_t, x_t, b_t, c_t = inputs
        state = jnp.exp(step_t[None, :] * rate) * state + b_t[:, None] * (step_t * x_t)[None, :]
        return (state, lax.optimization_barrier(jnp.sum(c_t[:, None] * state, axis=0)))
    _, outputs = lax.scan(advance, jnp.zeros((STATE, INNER), jnp.float32), (step, xfloat, bmat, cmat))
    y_out = (outputs + skip[None, :] * xfloat).astype(jnp.bfloat16)
    y_out = lax.optimization_barrier(y_out)
    return (y_out.astype(jnp.float32) * jax.nn.silu(gate_input.astype(jnp.float32))).astype(jnp.bfloat16)
```

```python
import functools

import jax
import jax.numpy as jnp
from jax import lax
from jax.experimental import pallas as pl
from jax.experimental.pallas import tpu as pltpu
from jax.sharding import PartitionSpec as P

LOG2E = 1.4426950408889634
LANES = 128
F32 = jnp.float32
BF16 = jnp.bfloat16
VMEM_LIMIT = 48 * 1024 * 1024


def conv_proj_kernel(rows, width, states, x_ref, prior_ref, par_ref, xw_ref, xc_ref, proj_ref, bc_ref):
    shards, _, chans = par_ref.shape
    rank = proj_ref.shape[1]
    taps = states + 2
    halo = prior_ref.shape[0]

    @pl.when(pl.program_id(0) == 0)
    def _():
        proj_ref[...] = jnp.zeros_like(proj_ref)
        bc_ref[...] = jnp.zeros_like(bc_ref)

    for s in range(shards):
        at = slice(s * chans, (s + 1) * chans)
        full = jnp.concatenate([prior_ref[:, at].astype(F32), x_ref[:, at].astype(F32)], 0)
        total = jnp.broadcast_to(par_ref[s, taps + width : taps + width + 1, :], (rows, chans))
        for tap in range(width):
            start = halo - (width - 1) + tap
            total = total + par_ref[s, taps + tap : taps + tap + 1, :] * full[start : start + rows]
        xc = (total / (1.0 + jnp.exp(-total))).astype(BF16)
        xc_ref[:, at] = xc
        proj_ref[...] += jnp.dot(xc, xw_ref[s, :rank, :], preferred_element_type=F32)
        bc_ref[...] += lax.dot_general(
            xw_ref[s, rank:, :], xc, (((1,), (1,)), ((), ())), preferred_element_type=F32
        )


def spread(table_ref, turned):
    count, rows = turned.shape
    for t in range(rows):
        table_ref[t] = jnp.broadcast_to(turned[:, t : t + 1], (count, LANES))


def softplus(v):
    return jnp.maximum(v, 0.0) + jnp.log1p(jnp.exp(-jnp.abs(v)))


def step_kernel(states, proj_ref, bc_ref, gain_ref, dtw_ref, par_ref, xc_ref, step_ref, ends_ref,
                normed_ref, b_ref, drive_ref):
    shards, _, chans = dtw_ref.shape
    rows = proj_ref.shape[0]

    @pl.when(pl.program_id(0) == 0)
    def _():
        low = proj_ref[...]
        mean = jnp.mean(low * low, axis=1, keepdims=True)
        normed_ref[...] = (low * lax.rsqrt(mean + 1e-06) * gain_ref[...]).astype(BF16)
        spread(b_ref, bc_ref[:states])

    for s in range(shards):
        at = slice(s * chans, (s + 1) * chans)
        step = softplus(
            jnp.dot(normed_ref[...], dtw_ref[s], preferred_element_type=F32)
            + par_ref[s, states : states + 1, :]
        )
        step_ref[:, :, at] = step.reshape(rows // 8, 8, chans)
        drive = step * xc_ref[:, at].astype(F32)
        drive_ref[:, :, at] = drive.reshape(rows // 8, 8, chans)
        ends_ref[s, states : states + 8, :] = jnp.broadcast_to(
            jnp.sum(step, axis=0, keepdims=True), (8, chans)
        )
    pieces = [(s, l) for s in range(shards) for l in range(chans // LANES)]
    rates = [
        -LOG2E * jnp.exp(par_ref[s, :states, l * LANES : (l + 1) * LANES]) for s, l in pieces
    ]

    def advance(group, held):
        held = list(held)
        for r in range(8):
            b_now = b_ref[group * 8 + r]
            for i in range(len(pieces)):
                at = slice(i * LANES, (i + 1) * LANES)
                decay = jnp.exp2(step_ref[group, r : r + 1, at] * rates[i])
                held[i] = decay * held[i] + b_now * drive_ref[group, r : r + 1, at]
        return tuple(held)

    zero = jnp.zeros((states, LANES), F32)
    held = lax.fori_loop(0, rows // 8, advance, tuple(zero for _ in pieces))
    for i, (s, l) in enumerate(pieces):
        ends_ref[s, :states, l * LANES : (l + 1) * LANES] = held[i]


def gather_kernel(ny, nz, *refs):
    owns, outs = refs[:3], refs[3:6]
    send_sem, recv_sem, sib_sem = refs[6:]
    seq = lax.axis_index("seq")
    batch = lax.axis_index("batch")
    core = lax.rem(batch, 2)
    y, z = seq // nz, lax.rem(seq, nz)
    sibling = batch + 1 - 2 * core

    def place(yy, zz):
        return lax.rem(yy + ny, ny) * nz + lax.rem(zz + nz, nz)

    barrier = pltpu.get_barrier_semaphore()
    for there in (place(y + 1, z), place(y - 1, z), place(y, z + 1), place(y, z - 1)):
        pl.semaphore_signal(barrier, inc=1, device_id={"seq": there},
                            device_id_type=pl.DeviceIdType.MESH)
    pl.semaphore_signal(barrier, inc=1, device_id={"batch": sibling},
                        device_id_type=pl.DeviceIdType.MESH)
    pl.semaphore_wait(barrier, 5)

    def route(first, second, where, h):
        copies = []

        def source(part, fo, so):
            if fo == 0 and so == 0:
                size = owns[part].shape[0] // 2
                return owns[part].at[pl.ds(h * size, size)]
            return outs[part].at[where(fo, so), pl.ds(h * (outs[part].shape[1] // 2),
                                                      outs[part].shape[1] // 2)]

        def target(part, fo, so):
            size = outs[part].shape[1] // 2
            return outs[part].at[where(fo, so), pl.ds(h * size, size)]

        def push(part, fo, so, df, ds):
            copy = pltpu.make_async_remote_copy(
                src_ref=source(part, fo, so),
                dst_ref=target(part, fo, so),
                send_sem=send_sem.at[len(copies)],
                recv_sem=recv_sem.at[part, where(fo, so)],
                device_id={"seq": where(df, ds)},
                device_id_type=pl.DeviceIdType.MESH,
            )
            copy.start()
            copies.append(copy)

        def share(part, fo, so):
            copy = pltpu.make_async_remote_copy(
                src_ref=target(part, fo, so),
                dst_ref=target(part, fo, so),
                send_sem=send_sem.at[len(copies)],
                recv_sem=sib_sem.at[part, where(fo, so)],
                device_id={"batch": sibling},
                device_id_type=pl.DeviceIdType.MESH,
            )
            copy.start()
            copies.append(copy)

        def arrive(part, fo, so, sem):
            pltpu.make_async_remote_copy(
                src_ref=target(part, fo, so),
                dst_ref=target(part, fo, so),
                send_sem=send_sem.at[0],
                recv_sem=sem.at[part, where(fo, so)],
                device_id={"batch": sibling},
                device_id_type=pl.DeviceIdType.MESH,
            ).wait_recv()

        reach = {1: first // 2, -1: first - 1 - first // 2}

        def second_reach(fo, way):
            longer = second // 2 if fo % 2 == 0 else second - 1 - second // 2
            return longer if way == 1 else second - 1 - longer

        def launch_second(part, fo):
            for way in (1, -1):
                push(part, fo, 0, 0, way)

        def advance_second(part, fo, d):
            for way in (1, -1):
                if d <= second_reach(fo, way):
                    arrive(part, fo, -way * d, recv_sem)
                    if d < second_reach(fo, way):
                        push(part, fo, -way * d, 0, way)
                    share(part, fo, -way * d)

        for part in range(3):
            for way in (1, -1):
                push(part, 0, 0, way, 0)
            if part < 2:
                launch_second(part, 0)
        order = [0]
        for d in range(1, max(reach.values()) + 1):
            for part in range(3):
                for way in (1, -1):
                    if d <= reach[way]:
                        arrive(part, -way * d, 0, recv_sem)
                        if d < reach[way]:
                            push(part, -way * d, 0, way, 0)
                        if part < 2:
                            launch_second(part, -way * d)
                        share(part, -way * d, 0)
                        if part == 0:
                            order.append(-way * d)
        steps = max(second_reach(fo, way) for fo in order for way in (1, -1))
        for d in range(1, steps + 2):
            for fo in order:
                if d <= steps:
                    for part in range(2):
                        advance_second(part, fo, d)
                if d == 1:
                    launch_second(2, fo)
                else:
                    advance_second(2, fo, d - 1)
        for copy in copies:
            copy.wait_send()

    @pl.when(core == 0)
    def _():
        route(nz, ny, lambda fo, so: place(y + so, z + fo), 0)

    @pl.when(core == 1)
    def _():
        route(ny, nz, lambda fo, so: place(y + fo, z + so), 1)

    for part in range(3):
        outs[part][seq] = owns[part][...]

        def collect(k, carry):
            at = lax.rem(seq + k, ny * nz)
            size = outs[part].shape[1] // 2
            dst = outs[part].at[at, pl.ds(pl.multiple_of((1 - core) * size, size), size)]
            pltpu.make_async_remote_copy(
                src_ref=dst,
                dst_ref=dst,
                send_sem=send_sem.at[0],
                recv_sem=sib_sem.at[part, at],
                device_id={"batch": sibling},
                device_id_type=pl.DeviceIdType.MESH,
            ).wait_recv()
            return carry

        lax.fori_loop(1, ny * nz, collect, 0)


def exchange_kernel(states, ends_ref, alog_ref, starts_ref, held_ref, back_ref,
                    send_sem, recv_sem, send2_sem, recv2_sem):
    count, _, chans = ends_ref.shape
    me = lax.axis_index("seq")

    barrier = pltpu.get_barrier_semaphore()

    def greet(k, carry):
        pl.semaphore_signal(barrier, inc=1, device_id={"seq": lax.rem(me + k, count)},
                            device_id_type=pl.DeviceIdType.MESH)
        return carry

    lax.fori_loop(1, count, greet, 0)
    pl.semaphore_wait(barrier, count - 1)

    def out_copy(k):
        there = lax.rem(me + k, count)
        return pltpu.make_async_remote_copy(
            src_ref=ends_ref.at[there],
            dst_ref=held_ref.at[me],
            send_sem=send_sem.at[k],
            recv_sem=recv_sem.at[k],
            device_id={"seq": there},
            device_id_type=pl.DeviceIdType.MESH,
        )

    def back_copy(k):
        there = lax.rem(me + k, count)
        return pltpu.make_async_remote_copy(
            src_ref=back_ref.at[there],
            dst_ref=starts_ref.at[me],
            send_sem=send2_sem.at[k],
            recv_sem=recv2_sem.at[k],
            device_id={"seq": there},
            device_id_type=pl.DeviceIdType.MESH,
        )

    def in_wait(k, into, sem):
        source = lax.rem(me - k + count, count)
        pltpu.make_async_remote_copy(
            src_ref=into.at[source],
            dst_ref=into.at[source],
            send_sem=sem.at[k],
            recv_sem=sem.at[k],
            device_id={"seq": source},
            device_id_type=pl.DeviceIdType.MESH,
        ).wait_recv()

    def loop(step):
        def body(k, carry):
            step(k)
            return carry

        lax.fori_loop(1, count, body, 0)

    loop(lambda k: out_copy(k).start())
    held_ref[me] = ends_ref[me]
    rates = -LOG2E * jnp.exp(alog_ref[...])
    loop(lambda k: in_wait(k, held_ref, recv_sem))

    def link(i, held):
        back_ref[i] = held
        decay = jnp.exp2(held_ref[i, states : states + 1, :] * rates)
        return decay * held + held_ref[i, :states, :]

    lax.fori_loop(0, count, link, jnp.zeros((states, chans), F32))
    loop(lambda k: back_copy(k).start())
    starts_ref[me] = back_ref[me]
    loop(lambda k: out_copy(k).wait_send())
    loop(lambda k: in_wait(k, starts_ref, recv2_sem))
    loop(lambda k: back_copy(k).wait_send())


def scan_kernel(states, bc_ref, step_ref, xc_ref, gate_ref, par_ref, starts_ref, out_ref,
                b_ref, c_ref, drive_ref, part_ref):
    shards, _, chans = par_ref.shape
    rows = gate_ref.shape[0]

    @pl.when(pl.program_id(0) == 0)
    def _():
        spread(b_ref, bc_ref[:states])
        spread(c_ref, bc_ref[states:])

    drive_ref[...] = step_ref[...] * xc_ref[...].astype(F32).reshape(drive_ref.shape)
    pieces = [(s, l) for s in range(shards) for l in range(chans // LANES)]
    rates = [
        -LOG2E * jnp.exp(par_ref[s, :states, l * LANES : (l + 1) * LANES]) for s, l in pieces
    ]

    def advance(group, held):
        held = list(held)
        for r in range(8):
            t = group * 8 + r
            b_now = b_ref[t]
            c_now = c_ref[t]
            for i in range(len(pieces)):
                at = slice(i * LANES, (i + 1) * LANES)
                decay = jnp.exp2(step_ref[group, r : r + 1, at] * rates[i])
                held[i] = decay * held[i] + b_now * drive_ref[group, r : r + 1, at]
                seen = c_now * held[i]
                part_ref[i, pl.ds(pl.multiple_of(t * 8, 8), 8), :] = seen[:8] + seen[8:]
        return tuple(held)

    held = tuple(starts_ref[s, :, l * LANES : (l + 1) * LANES] for s, l in pieces)
    lax.fori_loop(0, rows // 8, advance, held)
    for i, (s, l) in enumerate(pieces):
        at = slice(i * LANES, (i + 1) * LANES)
        total = part_ref[i, pl.ds(0, rows, stride=8), :]
        for k in range(1, 8):
            total = total + part_ref[i, pl.ds(k, rows, stride=8), :]
        skip = par_ref[s, states + 1 : states + 2, l * LANES : (l + 1) * LANES]
        y_out = (total + skip * xc_ref[:, at].astype(F32)).astype(BF16).astype(F32)
        gate = gate_ref[:, at].astype(F32)
        out_ref[:, at] = (y_out * (gate / (1.0 + jnp.exp(-gate)))).astype(BF16)


def local(
    conv_input,
    gate_input,
    conv_weight,
    conv_bias,
    x_weight,
    dt_gain,
    dt_weight,
    dt_bias,
    a_log,
    skip,
):
    width = conv_weight.shape[0]
    rank = dt_weight.shape[0]
    states, chans = a_log.shape
    rows, inner = conv_input.shape
    count = lax.axis_size("seq")
    proj_cols = x_weight.shape[1]
    shards = 2
    block = shards * chans
    grid = inner // block
    params = pltpu.CompilerParams(
        dimension_semantics=("arbitrary",), vmem_limit_bytes=VMEM_LIMIT
    )

    prior = lax.ppermute(
        conv_input[rows - 8 :], "seq", [(i, i + 1) for i in range(count - 1)]
    )
    par_rows = 32
    par = jnp.concatenate(
        [
            a_log,
            dt_bias[None, :],
            skip[None, :],
            conv_weight.astype(F32),
            conv_bias.astype(F32)[None, :],
            jnp.zeros((par_rows - states - 2 - width - 1, chans), F32),
        ],
        0,
    )
    xw = jnp.concatenate([x_weight[:, :rank], x_weight[:, rank:].T], 0)
    xw_rows = xw.shape[0]
    ny, nz = 4, count // 4
    copies = 6 * (count - 1)
    vmem = pl.BlockSpec(memory_space=pltpu.VMEM)
    par, xw, dtw = pl.pallas_call(
        functools.partial(gather_kernel, ny, nz),
        in_specs=[vmem] * 3,
        out_specs=[vmem] * 3,
        out_shape=[
            jax.ShapeDtypeStruct((count, par_rows, chans), F32),
            jax.ShapeDtypeStruct((count, xw_rows, chans), BF16),
            jax.ShapeDtypeStruct((count, rank, chans), BF16),
        ],
        scratch_shapes=[
            pltpu.SemaphoreType.DMA((copies,)),
            pltpu.SemaphoreType.DMA((3, count)),
            pltpu.SemaphoreType.DMA((3, count)),
        ],
        compiler_params=pltpu.CompilerParams(
            collective_id=0, has_side_effects=True, vmem_limit_bytes=VMEM_LIMIT
        ),
        name="gather",
    )(par, xw, dt_weight)

    whole = lambda *shape: pl.BlockSpec(shape, lambda i: (0,) * len(shape))
    columns = lambda height: pl.BlockSpec((height, block), lambda i: (0, i))
    stacked = lambda *shape: pl.BlockSpec((shards, *shape), lambda i: (i, 0, 0))
    tiled = pl.BlockSpec((rows // 8, 8, block), lambda i: (0, 0, i))

    xc, proj, bc = pl.pallas_call(
        functools.partial(conv_proj_kernel, rows, width, states),
        grid=(grid,),
        in_specs=[columns(rows), columns(8), stacked(par_rows, chans), stacked(xw_rows, chans)],
        out_specs=[columns(rows), whole(rows, rank), whole(2 * states, rows)],
        out_shape=[
            jax.ShapeDtypeStruct((rows, inner), BF16),
            jax.ShapeDtypeStruct((rows, rank), F32),
            jax.ShapeDtypeStruct((2 * states, rows), F32),
        ],
        compiler_params=params,
        cost_estimate=pl.CostEstimate(
            flops=700_000_000, bytes_accessed=9_000_000, transcendentals=2_000_000
        ),
        name="conv_proj",
    )(conv_input, prior, par, xw)

    step, ends = pl.pallas_call(
        functools.partial(step_kernel, states),
        grid=(grid,),
        in_specs=[
            whole(rows, rank),
            whole(2 * states, rows),
            whole(1, rank),
            stacked(rank, chans),
            stacked(par_rows, chans),
            columns(rows),
        ],
        out_specs=[tiled, stacked(states + 8, chans)],
        out_shape=[
            jax.ShapeDtypeStruct((rows // 8, 8, inner), F32),
            jax.ShapeDtypeStruct((count, states + 8, chans), F32),
        ],
        scratch_shapes=[
            pltpu.VMEM((rows, rank), BF16),
            pltpu.VMEM((rows, states, LANES), F32),
            pltpu.VMEM((rows // 8, 8, block), F32),
        ],
        compiler_params=params,
        cost_estimate=pl.CostEstimate(
            flops=700_000_000, bytes_accessed=11_000_000, transcendentals=18_000_000
        ),
        name="step_ends",
    )(proj, bc, dt_gain[None, :], dtw, par, xc)

    starts = pl.pallas_call(
        functools.partial(exchange_kernel, states),
        in_specs=[vmem] * 2,
        out_specs=vmem,
        out_shape=jax.ShapeDtypeStruct((count, states, chans), F32),
        scratch_shapes=[
            pltpu.VMEM((count, states + 8, chans), F32),
            pltpu.VMEM((count, states, chans), F32),
            *[pltpu.SemaphoreType.DMA((count,)) for _ in range(4)],
        ],
        compiler_params=pltpu.CompilerParams(
            collective_id=1, has_side_effects=True, vmem_limit_bytes=VMEM_LIMIT
        ),
        name="exchange",
    )(ends, a_log)

    return pl.pallas_call(
        functools.partial(scan_kernel, states),
        grid=(grid,),
        in_specs=[
            whole(2 * states, rows),
            tiled,
            columns(rows),
            columns(rows),
            stacked(par_rows, chans),
            stacked(states, chans),
        ],
        out_specs=columns(rows),
        out_shape=jax.ShapeDtypeStruct((rows, inner), BF16),
        scratch_shapes=[
            pltpu.VMEM((rows, states, LANES), F32),
            pltpu.VMEM((rows, states, LANES), F32),
            pltpu.VMEM((rows // 8, 8, block), F32),
            pltpu.VMEM((block // LANES, rows * 8, LANES), F32),
        ],
        compiler_params=params,
        cost_estimate=pl.CostEstimate(
            flops=100_000_000, bytes_accessed=11_000_000, transcendentals=18_000_000
        ),
        name="scan_gate",
    )(bc, step, xc, gate_input, par, starts)


def solution(mesh):
    return jax.shard_map(
        local,
        mesh=mesh,
        in_specs=(
            P(("batch", "seq"), None),
            P(("batch", "seq"), None),
            P(None, "seq"),
            P("seq"),
            P("seq", None),
            P(),
            P(None, "seq"),
            P("seq"),
            P(None, "seq"),
            P("seq"),
        ),
        out_specs=P(("batch", "seq"), None),
        check_vma=False,
    )
```

```python
import functools

import jax
import jax.numpy as jnp
from jax import lax
from jax.experimental import pallas as pl
from jax.experimental.pallas import tpu as pltpu
from jax.sharding import PartitionSpec as P

LOG2E = 1.4426950408889634
LANES = 128
F32 = jnp.float32
BF16 = jnp.bfloat16
VMEM_LIMIT = 60 * 1024 * 1024
PAR, XW, DTW = 0, 1, 2


def silu(v):
    return v / (1.0 + jnp.exp(-v))


def softplus(v):
    return jnp.maximum(v, 0.0) + jnp.log1p(jnp.exp(-jnp.abs(v)))


def spread(table_ref, turned):
    count, rows = turned.shape
    for t in range(rows):
        table_ref[t] = jnp.broadcast_to(turned[:, t : t + 1], (count, LANES))


def zigzag(j):
    return -(j + 1) // 2 if j % 2 else j // 2


class Route:
    def __init__(self, first, second, where, h, owns, outs, send_sem, recv_sem, sib_sem, sibling):
        self.first, self.second, self.where, self.h = first, second, where, h
        self.owns, self.outs = owns, outs
        self.send_sem, self.recv_sem, self.sib_sem = send_sem, recv_sem, sib_sem
        self.sibling = sibling
        self.sent = []
        self.reach = {1: first // 2, -1: first - 1 - first // 2}

    def target(self, part, fo, so):
        size = self.outs[part].shape[1] // 2
        return self.outs[part].at[self.where(fo, so), pl.ds(self.h * size, size)]

    def source(self, part, fo, so):
        if fo == 0 and so == 0:
            size = self.owns[part].shape[0] // 2
            return self.owns[part].at[pl.ds(self.h * size, size)]
        return self.target(part, fo, so)

    def send(self, part, fo, so, sem, device):
        pltpu.make_async_remote_copy(
            src_ref=self.source(part, fo, so),
            dst_ref=self.target(part, fo, so),
            send_sem=self.send_sem.at[len(self.sent)],
            recv_sem=sem.at[part, self.where(fo, so)],
            device_id=device,
            device_id_type=pl.DeviceIdType.MESH,
        ).start()
        self.sent.append(part)

    def push(self, part, fo, so, df, ds):
        self.send(part, fo, so, self.recv_sem, {"seq": self.where(df, ds)})

    def share(self, part, fo, so):
        self.send(part, fo, so, self.sib_sem, {"batch": self.sibling})

    def arrive(self, part, fo, so):
        pltpu.make_async_remote_copy(
            src_ref=self.target(part, fo, so),
            dst_ref=self.target(part, fo, so),
            send_sem=self.send_sem.at[0],
            recv_sem=self.recv_sem.at[part, self.where(fo, so)],
            device_id={"batch": self.sibling},
            device_id_type=pl.DeviceIdType.MESH,
        ).wait_recv()

    def drain(self):
        for i, part in enumerate(self.sent):
            pltpu.make_async_remote_copy(
                src_ref=self.target(part, 0, 0),
                dst_ref=self.target(part, 0, 0),
                send_sem=self.send_sem.at[i],
                recv_sem=self.recv_sem.at[part, self.where(0, 0)],
                device_id={"batch": self.sibling},
                device_id_type=pl.DeviceIdType.MESH,
            ).wait_send()

    def second_reach(self, fo, way):
        longer = self.second // 2 if fo % 2 == 0 else self.second - 1 - self.second // 2
        return longer if way == 1 else self.second - 1 - longer

    def launch_second(self, part, fo):
        for way in (1, -1):
            self.push(part, fo, 0, 0, way)

    def open(self):
        for part in (PAR, XW, DTW):
            for way in (1, -1):
                self.push(part, 0, 0, way, 0)
            if part != DTW:
                self.launch_second(part, 0)

    def first_step(self, d):
        for part in (PAR, XW, DTW):
            for way in (1, -1):
                if d <= self.reach[way]:
                    self.arrive(part, -way * d, 0)
                    if d < self.reach[way]:
                        self.push(part, -way * d, 0, way, 0)
                    if part != DTW:
                        self.launch_second(part, -way * d)
                    self.share(part, -way * d, 0)

    def second_step(self, part, fo, d, way):
        if d <= self.second_reach(fo, way):
            self.arrive(part, fo, -way * d)
            if d < self.second_reach(fo, way):
                self.push(part, fo, -way * d, 0, way)
            self.share(part, fo, -way * d)


class ZFirst(Route):
    def piece(self, parts, m):
        order = [zigzag(j) for j in range(self.first)]
        if m < self.first:
            for part in parts:
                for way in (1, -1):
                    self.second_step(part, order[m], 1, way)
        if 1 <= m:
            for d in range(2, self.second // 2 + 1):
                for part in parts:
                    for way in (1, -1):
                        self.second_step(part, order[m - 1], d, way)

    def launch(self, m):
        self.launch_second(DTW, zigzag(m))


class YFirst(Route):
    def piece(self, parts, m):
        if 1 <= m < self.second:
            so = zigzag(m)
            for part in parts:
                for j in range(self.first):
                    fo = zigzag(j)
                    way = -1 if so > 0 else 1
                    d = abs(so)
                    if d <= self.second_reach(fo, way):
                        self.second_step(part, fo, d, way)
                    elif so == -(self.second // 2):
                        self.second_step(part, fo, d, -way)

    def launch(self, m):
        if m < self.first:
            self.launch_second(DTW, zigzag(m))


def mixer_kernel(ny, nz, x_hbm, gate_hbm, cw_ref, cb_ref, xw_ref, gain_ref, dtw_ref, dtb_ref,
                 alog_ref, skip_ref, halo_ref, out_hbm,
                 x_ref, gate_ref, out_ref, prior_ref, parown_ref, xwown_ref, par_ref, xwall_ref,
                 dtwall_ref, xc_ref, proj_ref, bc_ref, normed_ref, b_ref, c_ref, step_ref,
                 drive_ref, part_ref, ends_ref, sums_ref, heldends_ref, heldsums_ref, back_ref,
                 starts_ref,
                 load_sem, store_sem, halo_sem, send_sem, recv_sem, sib_sem, ends_sem, sums_sem,
                 back_sem):
    count = ny * nz
    rows, inner = x_ref.shape
    width = cw_ref.shape[0]
    states, chans = alog_ref.shape
    rank = proj_ref.shape[1]
    taps = states + 2
    seq = lax.axis_index("seq")
    batch = lax.axis_index("batch")
    core = lax.rem(batch, 2)
    y, z = seq // nz, lax.rem(seq, nz)
    sibling = batch + 1 - 2 * core
    mesh_id = pl.DeviceIdType.MESH

    def place(yy, zz):
        return lax.rem(yy + ny, ny) * nz + lax.rem(zz + nz, nz)

    load_x = pltpu.make_async_copy(x_hbm, x_ref, load_sem.at[0])
    load_gate = pltpu.make_async_copy(gate_hbm, gate_ref, load_sem.at[1])
    load_x.start()
    load_gate.start()

    barrier = pltpu.get_barrier_semaphore()
    after, before = lax.rem(seq + 1, count), lax.rem(seq + count - 1, count)
    for there in (place(y + 1, z), place(y - 1, z), place(y, z + 1), place(y, z - 1), after,
                  before):
        pl.semaphore_signal(barrier, inc=1, device_id={"seq": there}, device_id_type=mesh_id)
    pl.semaphore_signal(barrier, inc=1, device_id={"batch": sibling}, device_id_type=mesh_id)

    parown_ref[...] = jnp.zeros_like(parown_ref)
    parown_ref[:states] = alog_ref[...]
    parown_ref[states : states + 1] = dtb_ref[...]
    parown_ref[states + 1 : states + 2] = skip_ref[...]
    parown_ref[taps : taps + width] = cw_ref[...].astype(F32)
    parown_ref[taps + width : taps + width + 1] = cb_ref[...].astype(F32)
    xwown_ref[:rank] = xw_ref[:, :rank]
    tail = xw_ref[:, rank:].astype(F32)
    tail = jnp.concatenate([tail, jnp.zeros((chans, LANES - tail.shape[1]), F32)], 1)
    xwown_ref[rank:] = tail.T[: 2 * states].astype(BF16)
    owns, outs = (parown_ref, xwown_ref, dtw_ref), (par_ref, xwall_ref, dtwall_ref)
    proj_ref[...] = jnp.zeros_like(proj_ref)
    bc_ref[...] = jnp.zeros_like(bc_ref)
    for part in (PAR, XW, DTW):
        outs[part][seq] = owns[part][...]

    pl.semaphore_wait(barrier, 7)
    shared = (owns, outs, send_sem, recv_sem, sib_sem, sibling)
    routes = (
        ZFirst(nz, ny, lambda fo, so: place(y + so, z + fo), 0, *shared),
        YFirst(ny, nz, lambda fo, so: place(y + fo, z + so), 1, *shared),
    )

    def both(act):
        for h in range(2):
            @pl.when(core == h)
            def _():
                act(routes[h])

    halo = pltpu.make_async_remote_copy(
        src_ref=halo_ref, dst_ref=prior_ref, send_sem=halo_sem.at[0], recv_sem=halo_sem.at[1],
        device_id={"seq": after}, device_id_type=mesh_id,
    )
    both(lambda r: r.open())
    halo.start()

    def silu_gate(i, carry):
        at = pl.ds(pl.multiple_of(i * chans, chans), chans)
        gate_ref[:, at] = silu(gate_ref[:, at].astype(F32)).astype(BF16)
        return carry

    def fill(d):
        pass

    load_x.wait()
    load_gate.wait()
    longest = max(r.reach[1] for r in routes)
    for d in range(1, longest + 1):
        both(lambda r: r.first_step(d))
        fill(d)
    halo.wait_recv()

    def sibling_wait(part, at):
        size = outs[part].shape[1] // 2
        dst = outs[part].at[at, pl.ds(pl.multiple_of((1 - core) * size, size), size)]
        pltpu.make_async_remote_copy(
            src_ref=dst, dst_ref=dst, send_sem=send_sem.at[0], recv_sem=sib_sem.at[part, at],
            device_id={"batch": sibling}, device_id_type=mesh_id,
        ).wait_recv()

    first_rows = jnp.where(seq > 0, 1.0, 0.0)

    def conv_shard(s):
        at = pl.ds(pl.multiple_of(s * chans, chans), chans)
        prior = prior_ref[:, at].astype(F32) * first_rows
        full = jnp.concatenate([jnp.zeros_like(prior), prior, x_ref[:, at].astype(F32)], 0)
        lead = 2 * prior.shape[0] - (width - 1)
        total = jnp.broadcast_to(par_ref[s, taps + width : taps + width + 1, :], (rows, chans))
        for tap in range(width):
            total = total + par_ref[s, taps + tap : taps + tap + 1, :] * full[
                lead + tap : lead + tap + rows
            ]
        xc = silu(total).astype(BF16)
        xc_ref[s] = xc
        proj_ref[...] += jnp.dot(xc, xwall_ref[s, :rank, :], preferred_element_type=F32)
        bc_ref[...] += lax.dot_general(
            xwall_ref[s, rank:, :], xc, (((1,), (1,)), ((), ())), preferred_element_type=F32
        )

    def pair(m, p):
        dz = jnp.where(lax.rem(m, 2) == 1, -((m + 1) // 2), m // 2)
        return place(y + p, z + dz), place(y - p - 1 + ny, z + dz)

    def conv_group(m):
        def body(p, carry):
            sa, sb = pair(m, p)
            for j, s in enumerate((sa, sb)):
                if j == 0 and m == 0:
                    @pl.when(p > 0)
                    def _():
                        sibling_wait(PAR, s)
                        sibling_wait(XW, s)
                else:
                    sibling_wait(PAR, s)
                    sibling_wait(XW, s)
            conv_shard(sa)
            conv_shard(sb)
            return carry

        lax.fori_loop(0, ny // 2, body, 0)

    for m in range(nz + 1):
        def act(r):
            r.piece((PAR, XW), m)
            if m < nz:
                r.launch(m)
        both(act)
        if m > 0:
            conv_group(m - 1)

    low = proj_ref[...]
    mean = jnp.mean(low * low, axis=1, keepdims=True)
    normed_ref[...] = (low * lax.rsqrt(mean + 1e-06) * gain_ref[...]).astype(BF16)
    spread(b_ref, bc_ref[:states])

    blocks = chans // LANES

    def rates_of(s):
        return [
            -LOG2E * jnp.exp(par_ref[s, :states, l * LANES : (l + 1) * LANES])
            for l in range(blocks)
        ]

    def step_pair(sa, sb):
        for s in (sa, sb):
            step = softplus(
                jnp.dot(normed_ref[...], dtwall_ref[s], preferred_element_type=F32)
                + par_ref[s, states : states + 1, :]
            )
            step_ref[s] = step.reshape(rows // 8, 8, chans)
            drive_ref[s] = (step * xc_ref[s].astype(F32)).reshape(rows // 8, 8, chans)
            total = jnp.sum(step, axis=0, keepdims=True)
            for l in range(blocks):
                sums_ref[s, l : l + 1] = total[:, l * LANES : (l + 1) * LANES]
        pieces = [(s, l) for s in (sa, sb) for l in range(blocks)]
        rates = rates_of(sa) + rates_of(sb)

        def advance(group, held):
            held = list(held)
            for r in range(8):
                b_now = b_ref[group * 8 + r]
                for i, (s, l) in enumerate(pieces):
                    at = slice(l * LANES, (l + 1) * LANES)
                    decay = jnp.exp2(step_ref[s, group, r : r + 1, at] * rates[i])
                    held[i] = decay * held[i] + b_now * drive_ref[s, group, r : r + 1, at]
            return tuple(held)

        zero = jnp.zeros((states, LANES), F32)
        held = lax.fori_loop(0, rows // 8, advance, tuple(zero for _ in pieces))
        for i, (s, l) in enumerate(pieces):
            ends_ref[s, :, l * LANES : (l + 1) * LANES] = held[i].astype(BF16)

    def ends_copies(s, me):
        return (
            pltpu.make_async_remote_copy(
                src_ref=ends_ref.at[s], dst_ref=heldends_ref.at[me],
                send_sem=ends_sem.at[0, s], recv_sem=ends_sem.at[1, me],
                device_id={"seq": s}, device_id_type=mesh_id,
            ),
            pltpu.make_async_remote_copy(
                src_ref=sums_ref.at[s], dst_ref=heldsums_ref.at[me],
                send_sem=sums_sem.at[0, s], recv_sem=sums_sem.at[1, me],
                device_id={"seq": s}, device_id_type=mesh_id,
            ),
        )

    def send_ends(m):
        def body(p, carry):
            for j, s in enumerate(pair(m, p)):
                def go():
                    for copy in ends_copies(s, seq):
                        copy.start()
                if j == 0 and m == 0:
                    pl.when(p > 0)(go)
                else:
                    go()
            return carry

        lax.fori_loop(0, ny // 2, body, 0)

    def step_group(m):
        def body(p, carry):
            sa, sb = pair(m, p)
            for j, s in enumerate((sa, sb)):
                if j == 0 and m == 0:
                    @pl.when(p > 0)
                    def _():
                        sibling_wait(DTW, s)
                else:
                    sibling_wait(DTW, s)
            step_pair(sa, sb)
            return carry

        lax.fori_loop(0, ny // 2, body, 0)

    for m in range(nz + 1):
        both(lambda r: r.piece((DTW,), m))
        if m > 1:
            send_ends(m - 2)
        if m > 0:
            step_group(m - 1)
    spread(c_ref, bc_ref[states:])
    send_ends(nz - 1)
    heldends_ref[seq] = ends_ref[seq]
    heldsums_ref[seq] = sums_ref[seq]

    rates_own = [
        -LOG2E * jnp.exp(alog_ref[:, l * LANES : (l + 1) * LANES]) for l in range(blocks)
    ]

    def link(i, held):
        @pl.when(i != seq)
        def _():
            for copy in ends_copies(i, i):
                copy.wait_recv()
        out = []
        for l in range(blocks):
            at = slice(l * LANES, (l + 1) * LANES)
            back_ref[i, :, at] = held[l].astype(BF16)
            decay = jnp.exp2(heldsums_ref[i, l : l + 1] * rates_own[l])
            out.append(decay * held[l] + heldends_ref[i, :, at].astype(F32))
        return tuple(out)

    zero = jnp.zeros((states, LANES), F32)
    lax.fori_loop(0, count, link, tuple(zero for _ in range(blocks)))

    def back_copy(s, me):
        return pltpu.make_async_remote_copy(
            src_ref=back_ref.at[s], dst_ref=starts_ref.at[me],
            send_sem=back_sem.at[0, s], recv_sem=back_sem.at[1, me],
            device_id={"seq": s}, device_id_type=mesh_id,
        )

    def send_back(k, carry):
        m, j = k // ny, lax.rem(k, ny)
        dz = jnp.where(lax.rem(m, 2) == 1, -((m + 1) // 2), m // 2)
        dy = jnp.where(lax.rem(j, 2) == 1, -((j + 1) // 2), j // 2)
        back_copy(place(y - dy, z - dz), seq).start()
        return carry

    lax.fori_loop(1, count, send_back, 0)
    starts_ref[seq] = back_ref[seq]

    def out_copy(s):
        at = pl.ds(pl.multiple_of(s * chans, chans), chans)
        return pltpu.make_async_copy(out_ref.at[s], out_hbm.at[:, at], store_sem.at[s])

    def scan_pair(k, carry):
        m, p = k // (ny // 2), lax.rem(k, ny // 2)
        sa, sb = pair(m, p)

        @pl.when(k > 0)
        def _():
            for s in pair((k - 1) // (ny // 2), lax.rem(k - 1, ny // 2)):
                out_copy(s).start()
            back_copy(sa, sa).wait_recv()

        back_copy(sb, sb).wait_recv()
        pieces = [(s, l) for s in (sa, sb) for l in range(blocks)]
        rates = rates_of(sa) + rates_of(sb)

        def advance(group, held):
            held = list(held)
            for r in range(8):
                t = group * 8 + r
                b_now = b_ref[t]
                c_now = c_ref[t]
                for i, (s, l) in enumerate(pieces):
                    at = slice(l * LANES, (l + 1) * LANES)
                    decay = jnp.exp2(step_ref[s, group, r : r + 1, at] * rates[i])
                    held[i] = decay * held[i] + b_now * drive_ref[s, group, r : r + 1, at]
                    seen = c_now * held[i]
                    part_ref[i, pl.ds(pl.multiple_of(t * 8, 8), 8), :] = seen[:8] + seen[8:]
            return tuple(held)

        held = tuple(
            starts_ref[s, :, l * LANES : (l + 1) * LANES].astype(F32) for s, l in pieces
        )
        lax.fori_loop(0, rows // 8, advance, held)
        for i, (s, l) in enumerate(pieces):
            at = slice(l * LANES, (l + 1) * LANES)
            total = part_ref[i, pl.ds(0, rows, stride=8), :]
            for r in range(1, 8):
                total = total + part_ref[i, pl.ds(r, rows, stride=8), :]
            skip = par_ref[s, states + 1 : states + 2, at]
            y_out = (total + skip * xc_ref[s, :, at].astype(F32)).astype(BF16).astype(F32)
            wide = pl.ds(pl.multiple_of(s * chans + l * LANES, LANES), LANES)
            gate = gate_ref[:, wide].astype(F32)
            out_ref[s, :, at] = (y_out * silu(gate)).astype(BF16)
        return carry

    pairs = count // 2
    lax.fori_loop(0, pairs, scan_pair, 0)
    both(lambda r: r.drain())
    halo.wait_send()

    def finish(k, carry):
        s = lax.rem(seq + k, count)
        for copy in ends_copies(s, s):
            copy.wait_send()
        back_copy(s, s).wait_send()
        return carry

    lax.fori_loop(1, count, finish, 0)
    for s in pair((pairs - 1) // (ny // 2), (pairs - 1) % (ny // 2)):
        out_copy(s).start()

    def stored(s, carry):
        out_copy(s).wait()
        return carry

    lax.fori_loop(0, count, stored, 0)


def local(
    conv_input,
    gate_input,
    conv_weight,
    conv_bias,
    x_weight,
    dt_gain,
    dt_weight,
    dt_bias,
    a_log,
    skip,
):
    width = conv_weight.shape[0]
    rank = dt_weight.shape[0]
    states, chans = a_log.shape
    rows, inner = conv_input.shape
    count = lax.axis_size("seq")
    ny, nz = 4, count // 4
    par_rows = 32
    xw_rows = rank + 2 * states
    dma = pltpu.SemaphoreType.DMA
    vmem = pl.BlockSpec(memory_space=pltpu.VMEM)
    hbm = pl.BlockSpec(memory_space=pl.ANY)
    return pl.pallas_call(
        functools.partial(mixer_kernel, ny, nz),
        in_specs=[hbm, hbm] + [vmem] * 9,
        out_specs=hbm,
        out_shape=jax.ShapeDtypeStruct((rows, inner), BF16),
        scratch_shapes=[
            pltpu.VMEM((rows, inner), BF16),
            pltpu.VMEM((rows, inner), BF16),
            pltpu.VMEM((count, rows, chans), BF16),
            pltpu.VMEM((4, inner), BF16),
            pltpu.VMEM((par_rows, chans), F32),
            pltpu.VMEM((xw_rows, chans), BF16),
            pltpu.VMEM((count, par_rows, chans), F32),
            pltpu.VMEM((count, xw_rows, chans), BF16),
            pltpu.VMEM((count, rank, chans), BF16),
            pltpu.VMEM((count, rows, chans), BF16),
            pltpu.VMEM((rows, rank), F32),
            pltpu.VMEM((2 * states, rows), F32),
            pltpu.VMEM((rows, rank), BF16),
            pltpu.VMEM((rows, states, LANES), F32),
            pltpu.VMEM((rows, states, LANES), F32),
            pltpu.VMEM((count, rows // 8, 8, chans), F32),
            pltpu.VMEM((count, rows // 8, 8, chans), F32),
            pltpu.VMEM((2 * chans // LANES, rows * 8, LANES), F32),
            pltpu.VMEM((count, states, chans), BF16),
            pltpu.VMEM((count, chans // LANES, LANES), F32),
            pltpu.VMEM((count, states, chans), BF16),
            pltpu.VMEM((count, chans // LANES, LANES), F32),
            pltpu.VMEM((count, states, chans), BF16),
            pltpu.VMEM((count, states, chans), BF16),
            dma((2,)),
            dma((count,)),
            dma((2,)),
            dma((6 * (count - 1),)),
            dma((3, count)),
            dma((3, count)),
            dma((2, count)),
            dma((2, count)),
            dma((2, count)),
        ],
        compiler_params=pltpu.CompilerParams(
            collective_id=0, has_side_effects=True, vmem_limit_bytes=VMEM_LIMIT
        ),
        name="mixer",
    )(
        conv_input,
        gate_input,
        conv_weight,
        conv_bias[None, :],
        x_weight,
        dt_gain[None, :],
        dt_weight,
        dt_bias[None, :],
        a_log,
        skip[None, :],
        conv_input[rows - 4 :],
    )


def solution(mesh):
    return jax.shard_map(
        local,
        mesh=mesh,
        in_specs=(
            P(("batch", "seq"), None),
            P(("batch", "seq"), None),
            P(None, "seq"),
            P("seq"),
            P("seq", None),
            P(),
            P(None, "seq"),
            P("seq"),
            P(None, "seq"),
            P("seq"),
        ),
        out_specs=P(("batch", "seq"), None),
        check_vma=False,
    )
```

```python
import functools

import jax
import jax.numpy as jnp
from jax import lax
from jax.experimental import pallas as pl
from jax.experimental.pallas import tpu as pltpu
from jax.sharding import PartitionSpec as P

LOG2E = 1.4426950408889634
LANES = 128
F32 = jnp.float32
BF16 = jnp.bfloat16
VMEM_LIMIT = 60 * 1024 * 1024
PAR, XW, DTW = 0, 1, 2


def silu(v):
    return v / (1.0 + jnp.exp(-v))


def softplus(v):
    return jnp.maximum(v, 0.0) + jnp.log1p(jnp.exp(-jnp.abs(v)))


def spread(table_ref, turned):
    count, rows = turned.shape
    for t in range(rows):
        table_ref[t] = jnp.broadcast_to(turned[:, t : t + 1], (count, LANES))


def zigzag(j):
    return -(j + 1) // 2 if j % 2 else j // 2


class Route:
    def __init__(self, first, second, where, h, owns, outs, send_sem, recv_sem, sib_sem, sibling,
                 offer, quarter):
        self.offer, self.quarter = offer, quarter
        self.first, self.second, self.where, self.h = first, second, where, h
        self.owns, self.outs = owns, outs
        self.send_sem, self.recv_sem, self.sib_sem = send_sem, recv_sem, sib_sem
        self.sibling = sibling
        self.sent = []
        self.reach = {1: first // 2, -1: first - 1 - first // 2}

    def span(self, part):
        rows = self.outs[part].shape[1]
        if part == DTW:
            size = rows // 8
            return pl.ds(pl.multiple_of(self.h * (rows // 2) + self.quarter * size, size), size)
        return pl.ds(self.h * (rows // 2), rows // 2)

    def target(self, part, fo, so):
        return self.outs[part].at[self.where(fo, so), self.span(part)]

    def source(self, part, fo, so):
        if fo == 0 and so == 0:
            return self.owns[part].at[self.span(part)]
        return self.target(part, fo, so)

    def send(self, part, fo, so, sem, device):
        pltpu.make_async_remote_copy(
            src_ref=self.source(part, fo, so),
            dst_ref=self.target(part, fo, so),
            send_sem=self.send_sem.at[len(self.sent)],
            recv_sem=sem.at[part, self.where(fo, so)],
            device_id=device,
            device_id_type=pl.DeviceIdType.MESH,
        ).start()
        self.sent.append(part)

    def push(self, part, fo, so, df, ds):
        self.send(part, fo, so, self.recv_sem, {"seq": self.where(df, ds)})

    def share(self, part, fo, so):
        if part == DTW:
            self.offer(self.target(part, fo, so), self.where(fo, so))
            return
        self.send(part, fo, so, self.sib_sem, {"batch": self.sibling})

    def arrive(self, part, fo, so):
        pltpu.make_async_remote_copy(
            src_ref=self.target(part, fo, so),
            dst_ref=self.target(part, fo, so),
            send_sem=self.send_sem.at[0],
            recv_sem=self.recv_sem.at[part, self.where(fo, so)],
            device_id={"batch": self.sibling},
            device_id_type=pl.DeviceIdType.MESH,
        ).wait_recv()

    def drain(self):
        for i, part in enumerate(self.sent):
            pltpu.make_async_remote_copy(
                src_ref=self.target(part, 0, 0),
                dst_ref=self.target(part, 0, 0),
                send_sem=self.send_sem.at[i],
                recv_sem=self.recv_sem.at[part, self.where(0, 0)],
                device_id={"batch": self.sibling},
                device_id_type=pl.DeviceIdType.MESH,
            ).wait_send()

    def straight(self, ring):
        return [zigzag(j) for j in range(1, ring)]


class ZFirst(Route):
    def launch(self, part, fo):
        for so in self.straight(self.second):
            self.push(part, fo, 0, 0, so)

    def open(self, parts):
        for part in parts:
            for way in (1, -1):
                self.push(part, 0, 0, way, 0)
            self.launch(part, 0)

    def round(self, parts, r):
        for part in parts:
            for way in (1, -1):
                if r <= self.reach[way]:
                    self.arrive(part, -way * r, 0)
                    if r < self.reach[way]:
                        self.push(part, -way * r, 0, way, 0)
                    self.launch(part, -way * r)
                    self.share(part, -way * r, 0)
        for part in parts:
            for fo in [zigzag(j) for j in range(self.first)]:
                if abs(fo) == r - 1:
                    for so in self.straight(self.second):
                        self.arrive(part, fo, so)
                        self.share(part, fo, so)


class YFirst(Route):
    def far(self, fo, way):
        longer = self.second // 2 if fo % 2 == 0 else self.second - 1 - self.second // 2
        return longer if way == 1 else self.second - 1 - longer

    def launch(self, part, fo):
        for way in (1, -1):
            self.push(part, fo, 0, 0, way)

    def open(self, parts):
        for part in parts:
            for fo in self.straight(self.first):
                self.push(part, 0, 0, fo, 0)
            self.launch(part, 0)

    def round(self, parts, r):
        if r == 1:
            for part in parts:
                for fo in self.straight(self.first):
                    self.arrive(part, fo, 0)
                    self.launch(part, fo)
                    self.share(part, fo, 0)
        for part in parts:
            for fo in [zigzag(j) for j in range(self.first)]:
                for way in (1, -1):
                    if r <= self.far(fo, way):
                        self.arrive(part, fo, -way * r)
                        if r < self.far(fo, way):
                            self.push(part, fo, -way * r, 0, way)
                        self.share(part, fo, -way * r)


def mixer_kernel(ny, nz, x_hbm, gate_hbm, cw_ref, cb_ref, xw_ref, gain_ref, dtw_ref, dtb_ref,
                 alog_ref, skip_ref, out_hbm,
                 tail_ref, halo_ref, x_ref, gate_ref, gated_ref, out_ref, prior_ref, parown_ref, par_ref, xwall_ref,
                 dtwall_ref, xc_ref, rate_ref, proj_ref, normed_ref, b_ref, c_ref, step_ref,
                 drive_ref, part_ref, ends_ref, sums_ref, heldends_ref, heldsums_ref, back_ref,
                 starts_ref,
                 load_sem, store_sem, halo_sem, send_sem, recv_sem, sib_sem, across_sem, hand_sem,
                 ends_sem, sums_sem, back_sem):
    count = ny * nz
    rows, inner = x_ref.shape
    width = cw_ref.shape[0]
    states, chans = alog_ref.shape
    rank = normed_ref.shape[1]
    taps = states + 2
    seq = lax.axis_index("seq")
    batch = lax.axis_index("batch")
    core = lax.rem(batch, 2)
    y, z = seq // nz, lax.rem(seq, nz)
    sibling = batch + 1 - 2 * core
    mesh_id = pl.DeviceIdType.MESH
    slab = batch // 2
    slabs = lax.axis_size("batch") // 2

    def beside(d):
        return lax.rem(slab + d, slabs) * 2 + core

    def place(yy, zz):
        return lax.rem(yy + ny, ny) * nz + lax.rem(zz + nz, nz)

    load_x = pltpu.make_async_copy(x_hbm, x_ref, load_sem.at[0])
    load_gate = pltpu.make_async_copy(gate_hbm, gate_ref, load_sem.at[1])
    load_tail = pltpu.make_async_copy(x_hbm.at[pl.ds(rows - 16, 16)], tail_ref, load_sem.at[2])
    load_tail.start()
    load_x.start()
    load_gate.start()

    barrier = pltpu.get_barrier_semaphore()
    after, before = lax.rem(seq + 1, count), lax.rem(seq + count - 1, count)
    for there in (place(y + 1, z), place(y - 1, z), place(y + 2, z), place(y, z + 1),
                  place(y, z - 1), after, before):
        pl.semaphore_signal(barrier, inc=1, device_id={"seq": there}, device_id_type=mesh_id)
    for there in (sibling, *(beside(d) for d in range(1, slabs))):
        pl.semaphore_signal(barrier, inc=1, device_id={"batch": there}, device_id_type=mesh_id)

    parown_ref[...] = jnp.zeros_like(parown_ref)
    parown_ref[:states] = alog_ref[...]
    parown_ref[states : states + 1] = dtb_ref[...]
    parown_ref[states + 1 : states + 2] = skip_ref[...]
    parown_ref[taps : taps + width] = cw_ref[...].astype(F32)
    parown_ref[taps + width : taps + width + 1] = cb_ref[...].astype(F32).reshape(1, chans)
    owns, outs = (parown_ref, xw_ref, dtw_ref), (par_ref, xwall_ref, dtwall_ref)
    proj_ref[...] = jnp.zeros_like(proj_ref)
    for part in (PAR, XW, DTW):
        outs[part][seq] = owns[part][...]

    load_tail.wait()
    halo_ref[...] = tail_ref[...].astype(F32)[16 - halo_ref.shape[0] :].astype(BF16)
    pl.semaphore_wait(barrier, 8 + slabs - 1)

    def across(ref, at, d):
        return pltpu.make_async_remote_copy(
            src_ref=ref, dst_ref=ref, send_sem=across_sem.at[0, d - 1, at],
            recv_sem=across_sem.at[1, d - 1, at], device_id={"batch": beside(d)},
            device_id_type=mesh_id,
        )

    def offer(ref, at):
        for d in range(1, slabs):
            across(ref, at, d).start()

    shared = (owns, outs, send_sem, recv_sem, sib_sem, sibling, offer, slab)
    routes = (
        ZFirst(nz, ny, lambda fo, so: place(y + so, z + fo), 0, *shared),
        YFirst(ny, nz, lambda fo, so: place(y + fo, z + so), 1, *shared),
    )

    def both(act):
        for h in range(2):
            @pl.when(core == h)
            def _():
                act(routes[h])

    halo = pltpu.make_async_remote_copy(
        src_ref=halo_ref, dst_ref=prior_ref, send_sem=halo_sem.at[0], recv_sem=halo_sem.at[1],
        device_id={"seq": after}, device_id_type=mesh_id,
    )
    both(lambda r: r.open((DTW, PAR, XW)))
    halo.start()
    load_gate.wait()

    def silu_gate(i, carry):
        at = pl.ds(pl.multiple_of(i * chans, chans), chans)
        gated_ref[i] = silu(gate_ref[:, at].astype(F32))
        return carry

    lax.fori_loop(0, count, silu_gate, 0)
    load_x.wait()
    halo.wait_recv()

    def sibling_wait(part, at):
        size = outs[part].shape[1] // 2
        dst = outs[part].at[at, pl.ds(pl.multiple_of((1 - core) * size, size), size)]
        pltpu.make_async_remote_copy(
            src_ref=dst, dst_ref=dst, send_sem=send_sem.at[0], recv_sem=sib_sem.at[part, at],
            device_id={"batch": sibling}, device_id_type=mesh_id,
        ).wait_recv()

    first_rows = jnp.where(seq > 0, 1.0, 0.0)

    def conv_shard(s):
        at = pl.ds(pl.multiple_of(s * chans, chans), chans)
        prior = prior_ref[:, at].astype(F32) * first_rows
        full = jnp.concatenate([jnp.zeros_like(prior), prior, x_ref[:, at].astype(F32)], 0)
        lead = 2 * prior.shape[0] - (width - 1)
        total = jnp.broadcast_to(par_ref[s, taps + width : taps + width + 1, :], (rows, chans))
        for tap in range(width):
            total = total + par_ref[s, taps + tap : taps + tap + 1, :] * full[
                lead + tap : lead + tap + rows
            ]
        xc = silu(total).astype(BF16)
        xc_ref[s] = xc
        rate_ref[s] = -LOG2E * jnp.exp(par_ref[s, :states])
        proj_ref[...] += lax.dot_general(
            xwall_ref[s], xc, (((1,), (1,)), ((), ())), preferred_element_type=F32
        )

    def pair(m, p):
        dz = jnp.where(lax.rem(m, 2) == 1, -((m + 1) // 2), m // 2)
        return place(y + p, z + dz), place(y - p - 1 + ny, z + dz)

    def kin(m, kind):
        dz = jnp.where(lax.rem(m, 2) == 1, -((m + 1) // 2), m // 2)
        same = lax.rem(y, 2) == kind
        return (place(y + jnp.where(same, 0, -1), z + dz),
                place(y + jnp.where(same, -2, 1), z + dz))

    def conv_group(m):
        def body(p, carry):
            sa, sb = pair(m, p)
            for j, s in enumerate((sa, sb)):
                if j == 0 and m == 0:
                    @pl.when(p > 0)
                    def _():
                        sibling_wait(PAR, s)
                        sibling_wait(XW, s)
                else:
                    sibling_wait(PAR, s)
                    sibling_wait(XW, s)
            conv_shard(sa)
            conv_shard(sb)
            return carry

        lax.fori_loop(0, ny // 2, body, 0)

    rounds = nz // 2 + 1
    groups = [[m for m in range(nz) if abs(zigzag(m)) == r - 1] for r in range(1, rounds + 1)]
    eighth = rank // 8

    def hand_over(m):
        def body(k, carry):
            sa, sb = pair(m, k // 2)
            at = jnp.where(lax.rem(k, 2) == 0, sa, sb)

            def go():
                for d in range(1, slabs):
                    there = lax.rem(slab - d + slabs, slabs)
                    dst = dtwall_ref.at[at, pl.ds(
                        pl.multiple_of(core * (rank // 2) + there * eighth, eighth), eighth)]
                    across(dst, at, d).wait_recv()
                hand(at).start()

            if m == 0:
                pl.when(k > 0)(go)
            else:
                go()
            return carry

        lax.fori_loop(0, ny, body, 0)

    def hand(at):
        half = dtwall_ref.at[at, pl.ds(pl.multiple_of(core * (rank // 2), rank // 2), rank // 2)]
        return pltpu.make_async_remote_copy(
            src_ref=half, dst_ref=half, send_sem=hand_sem.at[at], recv_sem=sib_sem.at[DTW, at],
            device_id={"batch": sibling}, device_id_type=mesh_id,
        )

    for r in range(1, rounds + 1):
        both(lambda route: route.round((DTW, PAR, XW), r))
        for m in groups[r - 1]:
            conv_group(m)
    hand_over(0)

    low = proj_ref[:rank]
    mean = jnp.mean(low * low, axis=0, keepdims=True)
    normed_ref[...] = ((low * lax.rsqrt(mean + 1e-06)).T * gain_ref[...]).astype(BF16)
    spread(b_ref, proj_ref[rank : rank + states])

    span = 16
    blocks = chans // LANES

    def rates_of(s):
        return [rate_ref[s, :, l * LANES : (l + 1) * LANES] for l in range(blocks)]

    def step_pair(sa, sb):
        for s in (sa, sb):
            step = softplus(
                jnp.dot(normed_ref[...], dtwall_ref[s], preferred_element_type=F32)
                + par_ref[s, states : states + 1, :]
            )
            step_ref[s] = step.reshape(rows // 8, 8, chans)
            drive_ref[s] = (step * xc_ref[s].astype(F32)).reshape(rows // 8, 8, chans)
            total = jnp.sum(step, axis=0, keepdims=True)
            for l in range(blocks):
                sums_ref[s, l : l + 1] = total[:, l * LANES : (l + 1) * LANES]
        pieces = [(s, l) for s in (sa, sb) for l in range(blocks)]
        rates = rates_of(sa) + rates_of(sb)

        def advance(g, held):
            held = list(held)
            for r in range(span):
                b_now = b_ref[g * span + r]
                group = g * (span // 8) + r // 8
                row = slice(r % 8, r % 8 + 1)
                for i, (s, l) in enumerate(pieces):
                    at = slice(l * LANES, (l + 1) * LANES)
                    decay = jnp.exp2(step_ref[s, group, row, at] * rates[i])
                    held[i] = decay * held[i] + b_now * drive_ref[s, group, row, at]
            return tuple(held)

        zero = jnp.zeros((states, LANES), F32)
        held = lax.fori_loop(0, rows // span, advance, tuple(zero for _ in pieces))
        for i, (s, l) in enumerate(pieces):
            ends_ref[s, :, l * LANES : (l + 1) * LANES] = held[i].astype(BF16)

    def ends_copies(s, me):
        return (
            pltpu.make_async_remote_copy(
                src_ref=ends_ref.at[s], dst_ref=heldends_ref.at[me],
                send_sem=ends_sem.at[0, s], recv_sem=ends_sem.at[1, me],
                device_id={"seq": s}, device_id_type=mesh_id,
            ),
            pltpu.make_async_remote_copy(
                src_ref=sums_ref.at[s], dst_ref=heldsums_ref.at[me],
                send_sem=sums_sem.at[0, s], recv_sem=sums_sem.at[1, me],
                device_id={"seq": s}, device_id_type=mesh_id,
            ),
        )

    def send_ends(m, kind):
        for s in kin(m, kind):
            @pl.when(s != seq)
            def _():
                for copy in ends_copies(s, seq):
                    copy.start()

    def step_kin(m, kind):
        sa, sb = kin(m, kind)
        for s in (sa, sb):
            @pl.when(s != seq)
            def _():
                sibling_wait(DTW, s)
        step_pair(sa, sb)

    rates_own = rates_of(seq)

    def link(i, held):
        @pl.when(i != seq)
        def _():
            for copy in ends_copies(i, i):
                copy.wait_recv()
        out = []
        for l in range(blocks):
            at = slice(l * LANES, (l + 1) * LANES)
            back_ref[i, :, at] = held[l].astype(BF16)
            decay = jnp.exp2(heldsums_ref[i, l : l + 1] * rates_own[l])
            out.append(decay * held[l] + heldends_ref[i, :, at].astype(F32))
        return tuple(out)

    def back_copy(s, me):
        return pltpu.make_async_remote_copy(
            src_ref=back_ref.at[s], dst_ref=starts_ref.at[me],
            send_sem=back_sem.at[0, s], recv_sem=back_sem.at[1, me],
            device_id={"seq": s}, device_id_type=mesh_id,
        )

    def send_back(k, carry):
        m, j = k // ny, lax.rem(k, ny)
        dz = jnp.where(lax.rem(m, 2) == 1, -((m + 1) // 2), m // 2)
        dy = jnp.where(lax.rem(j, 2) == 1, -((j + 1) // 2), j // 2)
        back_copy(place(y - dy, z - dz), seq).start()
        return carry

    def prefix():
        heldends_ref[seq] = ends_ref[seq]
        heldsums_ref[seq] = sums_ref[seq]
        zero = jnp.zeros((states, LANES), F32)
        lax.fori_loop(0, count, link, tuple(zero for _ in range(blocks)))
        starts_ref[seq] = back_ref[seq]
        lax.fori_loop(1, count, send_back, 0)

    for m in range(nz):
        if m + 1 < nz:
            hand_over(m + 1)
        if m > 0:
            send_ends(m - 1, 0)
        step_kin(m, 0)

    def later_kin(m, carry):
        send_ends(jnp.where(m == 0, nz - 1, m - 1), jnp.where(m == 0, 0, 1))
        step_kin(m, 1)
        return carry

    lax.fori_loop(0, nz // 2, later_kin, 0)
    spread(c_ref, proj_ref[rank + states :])
    pl.when(lax.rem(y, 2) == 0)(prefix)
    lax.fori_loop(nz // 2, nz, later_kin, 0)
    send_ends(nz - 1, 1)

    def out_copy(s):
        at = pl.ds(pl.multiple_of(s * chans, chans), chans)
        return pltpu.make_async_copy(out_ref.at[s], out_hbm.at[:, at], store_sem.at[s])

    def scan_pair(k, carry):
        sa, sb = kin(lax.rem(k, nz), k // nz)

        @pl.when(k > 0)
        def _():
            for s in kin(lax.rem(k - 1, nz), (k - 1) // nz):
                out_copy(s).start()

        for s in (sa, sb):
            @pl.when(s != seq)
            def _():
                back_copy(s, s).wait_recv()

        pieces = [(s, l) for s in (sa, sb) for l in range(blocks)]
        rates = rates_of(sa) + rates_of(sb)

        def advance(g, held):
            held = list(held)
            for r in range(span):
                t = g * span + r
                b_now = b_ref[t]
                c_now = c_ref[t]
                group = g * (span // 8) + r // 8
                row = slice(r % 8, r % 8 + 1)
                for i, (s, l) in enumerate(pieces):
                    at = slice(l * LANES, (l + 1) * LANES)
                    decay = jnp.exp2(step_ref[s, group, row, at] * rates[i])
                    held[i] = decay * held[i] + b_now * drive_ref[s, group, row, at]
                    seen = c_now * held[i]
                    part_ref[i, group, pl.ds(r % 8, 8, stride=8), :] = seen[:8] + seen[8:]
            return tuple(held)

        held = tuple(
            starts_ref[s, :, l * LANES : (l + 1) * LANES].astype(F32) for s, l in pieces
        )
        lax.fori_loop(0, rows // span, advance, held)
        for i, (s, l) in enumerate(pieces):
            at = slice(l * LANES, (l + 1) * LANES)
            total = part_ref[i, :, :8, :]
            for k in range(1, 8):
                total = total + part_ref[i, :, k * 8 : (k + 1) * 8, :]
            skip = par_ref[s, states + 1 : states + 2, at]
            y_out = total.reshape(rows, LANES) + skip * xc_ref[s, :, at].astype(F32)
            y_out = y_out.astype(BF16).astype(F32)
            out_ref[s, :, at] = (y_out * gated_ref[s, :, at]).astype(BF16)
        return carry

    pairs = count // 2
    lax.fori_loop(0, 3, scan_pair, 0)
    pl.when(lax.rem(y, 2) == 1)(prefix)
    lax.fori_loop(3, pairs, scan_pair, 0)
    both(lambda r: r.drain())
    halo.wait_send()

    def finish(k, carry):
        s = lax.rem(seq + k, count)
        for copy in ends_copies(s, s):
            copy.wait_send()
        back_copy(s, s).wait_send()
        hand(s).wait_send()
        small = dtwall_ref.at[s, pl.ds(0, eighth)]
        for d in range(1, slabs):
            across(small, s, d).wait_send()
        return carry

    lax.fori_loop(1, count, finish, 0)
    for s in kin(nz - 1, 1):
        out_copy(s).start()

    def stored(s, carry):
        out_copy(s).wait()
        return carry

    lax.fori_loop(0, count, stored, 0)


def local(
    conv_input,
    gate_input,
    conv_weight,
    conv_bias,
    x_weight,
    dt_gain,
    dt_weight,
    dt_bias,
    a_log,
    skip,
):
    width = conv_weight.shape[0]
    rank = dt_weight.shape[0]
    states, chans = a_log.shape
    rows, inner = conv_input.shape
    count = lax.axis_size("seq")
    ny, nz = 4, count // 4
    par_rows = 32
    xw_rows = rank + 2 * states
    dma = pltpu.SemaphoreType.DMA
    vmem = pl.BlockSpec(memory_space=pltpu.VMEM)
    hbm = pl.BlockSpec(memory_space=pl.ANY)
    return pl.pallas_call(
        functools.partial(mixer_kernel, ny, nz),
        in_specs=[hbm, hbm] + [vmem] * 8,
        out_specs=hbm,
        out_shape=jax.ShapeDtypeStruct((rows, inner), BF16),
        scratch_shapes=[
            pltpu.VMEM((16, inner), BF16),
            pltpu.VMEM((4, inner), BF16),
            pltpu.VMEM((rows, inner), BF16),
            pltpu.VMEM((rows, inner), BF16),
            pltpu.VMEM((count, rows, chans), F32),
            pltpu.VMEM((count, rows, chans), BF16),
            pltpu.VMEM((4, inner), BF16),
            pltpu.VMEM((par_rows, chans), F32),
            pltpu.VMEM((count, par_rows, chans), F32),
            pltpu.VMEM((count, xw_rows, chans), BF16),
            pltpu.VMEM((count, rank, chans), BF16),
            pltpu.VMEM((count, rows, chans), BF16),
            pltpu.VMEM((count, states, chans), F32),
            pltpu.VMEM((xw_rows, rows), F32),
            pltpu.VMEM((rows, rank), BF16),
            pltpu.VMEM((rows, states, LANES), F32),
            pltpu.VMEM((rows, states, LANES), F32),
            pltpu.VMEM((count, rows // 8, 8, chans), F32),
            pltpu.VMEM((count, rows // 8, 8, chans), F32),
            pltpu.VMEM((2 * chans // LANES, rows // 8, 64, LANES), F32),
            pltpu.VMEM((count, states, chans), BF16),
            pltpu.VMEM((count, chans // LANES, LANES), F32),
            pltpu.VMEM((count, states, chans), BF16),
            pltpu.VMEM((count, chans // LANES, LANES), F32),
            pltpu.VMEM((count, states, chans), BF16),
            pltpu.VMEM((count, states, chans), BF16),
            dma((3,)),
            dma((count,)),
            dma((2,)),
            dma((6 * (count - 1),)),
            dma((3, count)),
            dma((3, count)),
            dma((2, 3, count)),
            dma((count,)),
            dma((2, count)),
            dma((2, count)),
            dma((2, count)),
        ],
        compiler_params=pltpu.CompilerParams(
            collective_id=0, has_side_effects=True, vmem_limit_bytes=VMEM_LIMIT
        ),
        name="mixer",
    )(
        conv_input,
        gate_input,
        conv_weight,
        conv_bias,
        x_weight.T,
        dt_gain[None, :],
        dt_weight,
        dt_bias[None, :],
        a_log,
        skip[None, :],
    )


def solution(mesh):
    return jax.shard_map(
        local,
        mesh=mesh,
        in_specs=(
            P(("batch", "seq"), None),
            P(("batch", "seq"), None),
            P(None, "seq"),
            P("seq"),
            P("seq", None),
            P(),
            P(None, "seq"),
            P("seq"),
            P(None, "seq"),
            P("seq"),
        ),
        out_specs=P(("batch", "seq"), None),
        check_vma=False,
    )
```

```python
import functools

import jax
import jax.numpy as jnp
from jax import lax
from jax.experimental import pallas as pl
from jax.experimental.pallas import tpu as pltpu
from jax.sharding import PartitionSpec as P

LOG2E = 1.4426950408889634
LANES = 128
F32 = jnp.float32
BF16 = jnp.bfloat16
VMEM_LIMIT = 60 * 1024 * 1024
PAR, XW, DTW = 0, 1, 2


def silu(v):
    return v / (1.0 + jnp.exp(-v))


def softplus(v):
    return jnp.maximum(v, 0.0) + jnp.log1p(jnp.exp(-jnp.abs(v)))


def spread(table_ref, turned):
    count, rows = turned.shape
    for t in range(rows):
        table_ref[t] = jnp.broadcast_to(turned[:, t : t + 1], (count, LANES))


def zigzag(j):
    return -(j + 1) // 2 if j % 2 else j // 2


class Route:
    def __init__(self, first, second, where, h, owns, outs, send_sem, recv_sem, sib_sem, sibling,
                 offer, quarter):
        self.offer, self.quarter = offer, quarter
        self.first, self.second, self.where, self.h = first, second, where, h
        self.owns, self.outs = owns, outs
        self.send_sem, self.recv_sem, self.sib_sem = send_sem, recv_sem, sib_sem
        self.sibling = sibling
        self.sent = []
        self.reach = {1: first // 2, -1: first - 1 - first // 2}

    def span(self, part):
        rows = self.outs[part].shape[1]
        if part == DTW:
            size = rows // 8
            return pl.ds(pl.multiple_of(self.h * (rows // 2) + self.quarter * size, size), size)
        return pl.ds(self.h * (rows // 2), rows // 2)

    def target(self, part, fo, so):
        return self.outs[part].at[self.where(fo, so), self.span(part)]

    def source(self, part, fo, so):
        if fo == 0 and so == 0:
            return self.owns[part].at[self.span(part)]
        return self.target(part, fo, so)

    def send(self, part, fo, so, sem, device):
        pltpu.make_async_remote_copy(
            src_ref=self.source(part, fo, so),
            dst_ref=self.target(part, fo, so),
            send_sem=self.send_sem.at[len(self.sent)],
            recv_sem=sem.at[part, self.where(fo, so)],
            device_id=device,
            device_id_type=pl.DeviceIdType.MESH,
        ).start()
        self.sent.append(part)

    def push(self, part, fo, so, df, ds):
        self.send(part, fo, so, self.recv_sem, {"seq": self.where(df, ds)})

    def share(self, part, fo, so):
        if part == DTW:
            self.offer(self.target(part, fo, so), self.where(fo, so))
            return
        self.send(part, fo, so, self.sib_sem, {"batch": self.sibling})

    def arrive(self, part, fo, so):
        pltpu.make_async_remote_copy(
            src_ref=self.target(part, fo, so),
            dst_ref=self.target(part, fo, so),
            send_sem=self.send_sem.at[0],
            recv_sem=self.recv_sem.at[part, self.where(fo, so)],
            device_id={"batch": self.sibling},
            device_id_type=pl.DeviceIdType.MESH,
        ).wait_recv()

    def drain(self):
        for i, part in enumerate(self.sent):
            pltpu.make_async_remote_copy(
                src_ref=self.target(part, 0, 0),
                dst_ref=self.target(part, 0, 0),
                send_sem=self.send_sem.at[i],
                recv_sem=self.recv_sem.at[part, self.where(0, 0)],
                device_id={"batch": self.sibling},
                device_id_type=pl.DeviceIdType.MESH,
            ).wait_send()

    def end(self, part, fo, so):
        self.arrive(part, fo, so)
        self.share(part, fo, so)

    def straight(self, ring):
        return [zigzag(j) for j in range(1, ring)]


class ZFirst(Route):
    def launch(self, part, fo):
        for so in self.straight(self.second):
            self.push(part, fo, 0, 0, so)

    def open(self, parts):
        for part in parts:
            for way in (1, -1):
                self.push(part, 0, 0, way, 0)
            self.launch(part, 0)

    def near(self, part, r, way):
        self.arrive(part, -way * r, 0)
        if r < self.reach[way]:
            self.push(part, -way * r, 0, way, 0)
        self.launch(part, -way * r)
        self.share(part, -way * r, 0)

    def events(self, parts, r):
        found = []
        for part in parts:
            for way in (1, -1):
                if r <= self.reach[way]:
                    found.append(functools.partial(self.near, part, r, way))
        for part in parts:
            for fo in [zigzag(j) for j in range(self.first)]:
                if abs(fo) == r - 1:
                    for so in self.straight(self.second):
                        found.append(functools.partial(self.end, part, fo, so))
        return found


class YFirst(Route):
    def far(self, fo, way):
        longer = self.second // 2 if fo % 2 == 0 else self.second - 1 - self.second // 2
        return longer if way == 1 else self.second - 1 - longer

    def launch(self, part, fo):
        for way in (1, -1):
            self.push(part, fo, 0, 0, way)

    def open(self, parts):
        for part in parts:
            for fo in self.straight(self.first):
                self.push(part, 0, 0, fo, 0)
            self.launch(part, 0)

    def near(self, part, fo):
        self.arrive(part, fo, 0)
        self.launch(part, fo)
        self.share(part, fo, 0)

    def along(self, part, fo, r, way):
        self.arrive(part, fo, -way * r)
        if r < self.far(fo, way):
            self.push(part, fo, -way * r, 0, way)
        self.share(part, fo, -way * r)

    def events(self, parts, r):
        found = []
        if r == 1:
            for part in parts:
                for fo in self.straight(self.first):
                    found.append(functools.partial(self.near, part, fo))
        for part in parts:
            for fo in [zigzag(j) for j in range(self.first)]:
                for way in (1, -1):
                    if r <= self.far(fo, way):
                        found.append(functools.partial(self.along, part, fo, r, way))
        return found


def mixer_kernel(ny, nz, x_hbm, gate_hbm, cw_ref, cb_ref, xw_ref, gain_ref, dtw_ref, dtb_ref,
                 alog_ref, skip_ref, out_hbm,
                 tail_ref, halo_ref, x_ref, gate_ref, gated_ref, out_ref, prior_ref, parown_ref, par_ref, xwall_ref,
                 dtwall_ref, xc_ref, rate_ref, proj_ref, normed_ref, b_ref, c_ref, step_ref,
                 drive_ref, part_ref, ends_ref, sums_ref, heldends_ref, heldsums_ref, back_ref,
                 starts_ref,
                 load_sem, store_sem, halo_sem, send_sem, recv_sem, sib_sem, across_sem, hand_sem,
                 ends_sem, sums_sem, back_sem):
    count = ny * nz
    rows, inner = x_ref.shape
    width = cw_ref.shape[0]
    states, chans = alog_ref.shape
    rank = normed_ref.shape[1]
    taps = states + 2
    seq = lax.axis_index("seq")
    batch = lax.axis_index("batch")
    core = lax.rem(batch, 2)
    y, z = seq // nz, lax.rem(seq, nz)
    sibling = batch + 1 - 2 * core
    mesh_id = pl.DeviceIdType.MESH
    slab = batch // 2
    slabs = lax.axis_size("batch") // 2

    def beside(d):
        return lax.rem(slab + d, slabs) * 2 + core

    def place(yy, zz):
        return lax.rem(yy + ny, ny) * nz + lax.rem(zz + nz, nz)

    load_x = pltpu.make_async_copy(x_hbm, x_ref, load_sem.at[0])
    load_gate = pltpu.make_async_copy(gate_hbm, gate_ref, load_sem.at[1])
    load_tail = pltpu.make_async_copy(x_hbm.at[pl.ds(rows - 16, 16)], tail_ref, load_sem.at[2])
    load_tail.start()
    load_x.start()
    load_gate.start()

    barrier = pltpu.get_barrier_semaphore()
    after, before = lax.rem(seq + 1, count), lax.rem(seq + count - 1, count)
    for there in (place(y + 1, z), place(y - 1, z), place(y + 2, z), place(y, z + 1),
                  place(y, z - 1), after, before):
        pl.semaphore_signal(barrier, inc=1, device_id={"seq": there}, device_id_type=mesh_id)
    for there in (sibling, *(beside(d) for d in range(1, slabs))):
        pl.semaphore_signal(barrier, inc=1, device_id={"batch": there}, device_id_type=mesh_id)

    parown_ref[...] = jnp.zeros_like(parown_ref)
    parown_ref[:states] = alog_ref[...]
    parown_ref[states : states + 1] = dtb_ref[...]
    parown_ref[states + 1 : states + 2] = skip_ref[...]
    parown_ref[taps : taps + width] = cw_ref[...].astype(F32)
    parown_ref[taps + width : taps + width + 1] = cb_ref[...].astype(F32).reshape(1, chans)
    owns, outs = (parown_ref, xw_ref, dtw_ref), (par_ref, xwall_ref, dtwall_ref)
    proj_ref[...] = jnp.zeros_like(proj_ref)
    for part in (PAR, XW, DTW):
        outs[part][seq] = owns[part][...]

    load_tail.wait()
    halo_ref[...] = tail_ref[...].astype(F32)[16 - halo_ref.shape[0] :].astype(BF16)
    pl.semaphore_wait(barrier, 8 + slabs - 1)

    def across(ref, at, d):
        return pltpu.make_async_remote_copy(
            src_ref=ref, dst_ref=ref, send_sem=across_sem.at[0, d - 1, at],
            recv_sem=across_sem.at[1, d - 1, at], device_id={"batch": beside(d)},
            device_id_type=mesh_id,
        )

    def offer(ref, at):
        for d in range(1, slabs):
            across(ref, at, d).start()

    shared = (owns, outs, send_sem, recv_sem, sib_sem, sibling, offer, slab)
    routes = (
        ZFirst(nz, ny, lambda fo, so: place(y + so, z + fo), 0, *shared),
        YFirst(ny, nz, lambda fo, so: place(y + fo, z + so), 1, *shared),
    )

    def both(act):
        for h in range(2):
            @pl.when(core == h)
            def _():
                act(routes[h])

    halo = pltpu.make_async_remote_copy(
        src_ref=halo_ref, dst_ref=prior_ref, send_sem=halo_sem.at[0], recv_sem=halo_sem.at[1],
        device_id={"seq": after}, device_id_type=mesh_id,
    )
    both(lambda r: r.open((DTW, PAR, XW)))
    halo.start()

    def silu_gate(i, carry):
        at = pl.ds(pl.multiple_of(i * chans, chans), chans)
        gated_ref[i] = silu(gate_ref[:, at].astype(F32))
        return carry


    def sibling_wait(part, at):
        size = outs[part].shape[1] // 2
        dst = outs[part].at[at, pl.ds(pl.multiple_of((1 - core) * size, size), size)]
        pltpu.make_async_remote_copy(
            src_ref=dst, dst_ref=dst, send_sem=send_sem.at[0], recv_sem=sib_sem.at[part, at],
            device_id={"batch": sibling}, device_id_type=mesh_id,
        ).wait_recv()

    first_rows = jnp.where(seq > 0, 1.0, 0.0)

    def conv_shard(s):
        at = pl.ds(pl.multiple_of(s * chans, chans), chans)
        prior = prior_ref[:, at].astype(F32) * first_rows
        full = jnp.concatenate([jnp.zeros_like(prior), prior, x_ref[:, at].astype(F32)], 0)
        lead = 2 * prior.shape[0] - (width - 1)
        total = jnp.broadcast_to(par_ref[s, taps + width : taps + width + 1, :], (rows, chans))
        for tap in range(width):
            total = total + par_ref[s, taps + tap : taps + tap + 1, :] * full[
                lead + tap : lead + tap + rows
            ]
        xc = silu(total).astype(BF16)
        xc_ref[s] = xc
        rate_ref[s] = -LOG2E * jnp.exp(par_ref[s, :states])
        proj_ref[...] += lax.dot_general(
            xwall_ref[s], xc, (((1,), (1,)), ((), ())), preferred_element_type=F32
        )

    def pair(m, p):
        dz = jnp.where(lax.rem(m, 2) == 1, -((m + 1) // 2), m // 2)
        return place(y + p, z + dz), place(y - p - 1 + ny, z + dz)

    def kin(m, kind):
        dz = jnp.where(lax.rem(m, 2) == 1, -((m + 1) // 2), m // 2)
        same = lax.rem(y, 2) == kind
        return (place(y + jnp.where(same, 0, -1), z + dz),
                place(y + jnp.where(same, -2, 1), z + dz))

    def conv_pair(m, p):
        for j, s in enumerate(pair(m, p)):
            if m or p or j:
                sibling_wait(PAR, s)
                sibling_wait(XW, s)
            conv_shard(s)

    rounds = nz // 2 + 1
    groups = [[m for m in range(nz) if abs(zigzag(m)) == r - 1] for r in range(1, rounds + 1)]
    eighth = rank // 8

    def hand_over(m):
        def body(k, carry):
            sa, sb = pair(m, k // 2)
            at = jnp.where(lax.rem(k, 2) == 0, sa, sb)

            def go():
                for d in range(1, slabs):
                    there = lax.rem(slab - d + slabs, slabs)
                    dst = dtwall_ref.at[at, pl.ds(
                        pl.multiple_of(core * (rank // 2) + there * eighth, eighth), eighth)]
                    across(dst, at, d).wait_recv()
                hand(at).start()

            if m == 0:
                pl.when(k > 0)(go)
            else:
                go()
            return carry

        lax.fori_loop(0, ny, body, 0)

    def hand(at):
        half = dtwall_ref.at[at, pl.ds(pl.multiple_of(core * (rank // 2), rank // 2), rank // 2)]
        return pltpu.make_async_remote_copy(
            src_ref=half, dst_ref=half, send_sem=hand_sem.at[at], recv_sem=sib_sem.at[DTW, at],
            device_id={"batch": sibling}, device_id_type=mesh_id,
        )

    slots = 4
    waiting = []
    for r in range(1, rounds + 1):
        lists = [route.events((DTW, PAR, XW), r) for route in routes]
        for q in range(slots):
            for h in range(2):
                mine = lists[h][len(lists[h]) * q // slots : len(lists[h]) * (q + 1) // slots]
                if mine:
                    @pl.when(core == h)
                    def _():
                        for event in mine:
                            event()
            if r == 1:
                if q == 0:
                    load_gate.wait()
                lax.fori_loop(count * q // slots, count * (q + 1) // slots, silu_gate, 0)
            elif waiting:
                conv_pair(*waiting.pop(0))
        if r == 1:
            load_x.wait()
            halo.wait_recv()
        waiting += [(m, p) for m in groups[r - 1] for p in range(ny // 2)]
    hand_over(0)
    for m, p in waiting:
        conv_pair(m, p)

    low = proj_ref[:rank]
    mean = jnp.mean(low * low, axis=0, keepdims=True)
    normed_ref[...] = ((low * lax.rsqrt(mean + 1e-06)).T * gain_ref[...]).astype(BF16)
    spread(b_ref, proj_ref[rank : rank + states])

    span = 16
    blocks = chans // LANES

    def rates_of(s):
        return [rate_ref[s, :, l * LANES : (l + 1) * LANES] for l in range(blocks)]

    def step_pair(sa, sb):
        for s in (sa, sb):
            step = softplus(
                jnp.dot(normed_ref[...], dtwall_ref[s], preferred_element_type=F32)
                + par_ref[s, states : states + 1, :]
            )
            step_ref[s] = step.reshape(rows // 8, 8, chans)
            drive_ref[s] = (step * xc_ref[s].astype(F32)).reshape(rows // 8, 8, chans)
            total = jnp.sum(step, axis=0, keepdims=True)
            for l in range(blocks):
                sums_ref[s, l : l + 1] = total[:, l * LANES : (l + 1) * LANES]
        pieces = [(s, l) for s in (sa, sb) for l in range(blocks)]
        rates = rates_of(sa) + rates_of(sb)

        def advance(g, held):
            held = list(held)
            for r in range(span):
                b_now = b_ref[g * span + r]
                group = g * (span // 8) + r // 8
                row = slice(r % 8, r % 8 + 1)
                for i, (s, l) in enumerate(pieces):
                    at = slice(l * LANES, (l + 1) * LANES)
                    decay = jnp.exp2(step_ref[s, group, row, at] * rates[i])
                    held[i] = decay * held[i] + b_now * drive_ref[s, group, row, at]
            return tuple(held)

        zero = jnp.zeros((states, LANES), F32)
        held = lax.fori_loop(0, rows // span, advance, tuple(zero for _ in pieces))
        for i, (s, l) in enumerate(pieces):
            ends_ref[s, :, l * LANES : (l + 1) * LANES] = held[i].astype(BF16)

    def ends_copies(s, me):
        return (
            pltpu.make_async_remote_copy(
                src_ref=ends_ref.at[s], dst_ref=heldends_ref.at[me],
                send_sem=ends_sem.at[0, s], recv_sem=ends_sem.at[1, me],
                device_id={"seq": s}, device_id_type=mesh_id,
            ),
            pltpu.make_async_remote_copy(
                src_ref=sums_ref.at[s], dst_ref=heldsums_ref.at[me],
                send_sem=sums_sem.at[0, s], recv_sem=sums_sem.at[1, me],
                device_id={"seq": s}, device_id_type=mesh_id,
            ),
        )

    def send_ends(m, kind):
        for s in kin(m, kind):
            @pl.when(s != seq)
            def _():
                for copy in ends_copies(s, seq):
                    copy.start()

    def step_kin(m, kind):
        sa, sb = kin(m, kind)
        for s in (sa, sb):
            @pl.when(s != seq)
            def _():
                sibling_wait(DTW, s)
        step_pair(sa, sb)

    rates_own = rates_of(seq)

    def link(i, held):
        @pl.when(i != seq)
        def _():
            for copy in ends_copies(i, i):
                copy.wait_recv()
        out = []
        for l in range(blocks):
            at = slice(l * LANES, (l + 1) * LANES)
            back_ref[i, :, at] = held[l].astype(BF16)
            decay = jnp.exp2(heldsums_ref[i, l : l + 1] * rates_own[l])
            out.append(decay * held[l] + heldends_ref[i, :, at].astype(F32))
        return tuple(out)

    def back_copy(s, me):
        return pltpu.make_async_remote_copy(
            src_ref=back_ref.at[s], dst_ref=starts_ref.at[me],
            send_sem=back_sem.at[0, s], recv_sem=back_sem.at[1, me],
            device_id={"seq": s}, device_id_type=mesh_id,
        )

    def send_back(k, carry):
        m, j = k // ny, lax.rem(k, ny)
        dz = jnp.where(lax.rem(m, 2) == 1, -((m + 1) // 2), m // 2)
        dy = jnp.where(lax.rem(j, 2) == 1, -((j + 1) // 2), j // 2)
        back_copy(place(y - dy, z - dz), seq).start()
        return carry

    def prefix():
        heldends_ref[seq] = ends_ref[seq]
        heldsums_ref[seq] = sums_ref[seq]
        zero = jnp.zeros((states, LANES), F32)
        lax.fori_loop(0, count, link, tuple(zero for _ in range(blocks)))
        starts_ref[seq] = back_ref[seq]
        lax.fori_loop(1, count, send_back, 0)

    for m in range(nz):
        if m + 1 < nz:
            hand_over(m + 1)
        if m > 0:
            send_ends(m - 1, 0)
        step_kin(m, 0)

    def later_kin(m, carry):
        send_ends(jnp.where(m == 0, nz - 1, m - 1), jnp.where(m == 0, 0, 1))
        step_kin(m, 1)
        return carry

    lax.fori_loop(0, nz // 2 + 2, later_kin, 0)
    spread(c_ref, proj_ref[rank + states :])
    pl.when(lax.rem(y, 2) == 0)(prefix)
    lax.fori_loop(nz // 2 + 2, nz, later_kin, 0)
    send_ends(nz - 1, 1)

    def out_copy(s):
        at = pl.ds(pl.multiple_of(s * chans, chans), chans)
        return pltpu.make_async_copy(out_ref.at[s], out_hbm.at[:, at], store_sem.at[s])

    def scan_pair(k, carry):
        sa, sb = kin(lax.rem(k, nz), k // nz)

        @pl.when(k > 0)
        def _():
            for s in kin(lax.rem(k - 1, nz), (k - 1) // nz):
                out_copy(s).start()

        for s in (sa, sb):
            @pl.when(s != seq)
            def _():
                back_copy(s, s).wait_recv()

        pieces = [(s, l) for s in (sa, sb) for l in range(blocks)]
        rates = rates_of(sa) + rates_of(sb)

        def advance(g, held):
            held = list(held)
            for r in range(span):
                t = g * span + r
                b_now = b_ref[t]
                c_now = c_ref[t]
                group = g * (span // 8) + r // 8
                row = slice(r % 8, r % 8 + 1)
                for i, (s, l) in enumerate(pieces):
                    at = slice(l * LANES, (l + 1) * LANES)
                    decay = jnp.exp2(step_ref[s, group, row, at] * rates[i])
                    held[i] = decay * held[i] + b_now * drive_ref[s, group, row, at]
                    seen = c_now * held[i]
                    part_ref[i, group, pl.ds(r % 8, 8, stride=8), :] = seen[:8] + seen[8:]
            return tuple(held)

        held = tuple(
            starts_ref[s, :, l * LANES : (l + 1) * LANES].astype(F32) for s, l in pieces
        )
        lax.fori_loop(0, rows // span, advance, held)
        for i, (s, l) in enumerate(pieces):
            at = slice(l * LANES, (l + 1) * LANES)
            total = part_ref[i, :, :8, :]
            for k in range(1, 8):
                total = total + part_ref[i, :, k * 8 : (k + 1) * 8, :]
            skip = par_ref[s, states + 1 : states + 2, at]
            y_out = total.reshape(rows, LANES) + skip * xc_ref[s, :, at].astype(F32)
            y_out = y_out.astype(BF16).astype(F32)
            out_ref[s, :, at] = (y_out * gated_ref[s, :, at]).astype(BF16)
        return carry

    pairs = count // 2
    lax.fori_loop(0, 4, scan_pair, 0)
    pl.when(lax.rem(y, 2) == 1)(prefix)
    lax.fori_loop(4, pairs, scan_pair, 0)
    both(lambda r: r.drain())
    halo.wait_send()

    def finish(k, carry):
        s = lax.rem(seq + k, count)
        for copy in ends_copies(s, s):
            copy.wait_send()
        back_copy(s, s).wait_send()
        hand(s).wait_send()
        small = dtwall_ref.at[s, pl.ds(0, eighth)]
        for d in range(1, slabs):
            across(small, s, d).wait_send()
        return carry

    lax.fori_loop(1, count, finish, 0)
    for s in kin(nz - 1, 1):
        out_copy(s).start()

    def stored(s, carry):
        out_copy(s).wait()
        return carry

    lax.fori_loop(0, count, stored, 0)


def local(
    conv_input,
    gate_input,
    conv_weight,
    conv_bias,
    x_weight,
    dt_gain,
    dt_weight,
    dt_bias,
    a_log,
    skip,
):
    width = conv_weight.shape[0]
    rank = dt_weight.shape[0]
    states, chans = a_log.shape
    rows, inner = conv_input.shape
    count = lax.axis_size("seq")
    ny, nz = 4, count // 4
    par_rows = 32
    xw_rows = rank + 2 * states
    dma = pltpu.SemaphoreType.DMA
    vmem = pl.BlockSpec(memory_space=pltpu.VMEM)
    hbm = pl.BlockSpec(memory_space=pl.ANY)
    return pl.pallas_call(
        functools.partial(mixer_kernel, ny, nz),
        in_specs=[hbm, hbm] + [vmem] * 8,
        out_specs=hbm,
        out_shape=jax.ShapeDtypeStruct((rows, inner), BF16),
        scratch_shapes=[
            pltpu.VMEM((16, inner), BF16),
            pltpu.VMEM((4, inner), BF16),
            pltpu.VMEM((rows, inner), BF16),
            pltpu.VMEM((rows, inner), BF16),
            pltpu.VMEM((count, rows, chans), F32),
            pltpu.VMEM((count, rows, chans), BF16),
            pltpu.VMEM((4, inner), BF16),
            pltpu.VMEM((par_rows, chans), F32),
            pltpu.VMEM((count, par_rows, chans), F32),
            pltpu.VMEM((count, xw_rows, chans), BF16),
            pltpu.VMEM((count, rank, chans), BF16),
            pltpu.VMEM((count, rows, chans), BF16),
            pltpu.VMEM((count, states, chans), F32),
            pltpu.VMEM((xw_rows, rows), F32),
            pltpu.VMEM((rows, rank), BF16),
            pltpu.VMEM((rows, states, LANES), F32),
            pltpu.VMEM((rows, states, LANES), F32),
            pltpu.VMEM((count, rows // 8, 8, chans), F32),
            pltpu.VMEM((count, rows // 8, 8, chans), F32),
            pltpu.VMEM((2 * chans // LANES, rows // 8, 64, LANES), F32),
            pltpu.VMEM((count, states, chans), BF16),
            pltpu.VMEM((count, chans // LANES, LANES), F32),
            pltpu.VMEM((count, states, chans), BF16),
            pltpu.VMEM((count, chans // LANES, LANES), F32),
            pltpu.VMEM((count, states, chans), BF16),
            pltpu.VMEM((count, states, chans), BF16),
            dma((3,)),
            dma((count,)),
            dma((2,)),
            dma((6 * (count - 1),)),
            dma((3, count)),
            dma((3, count)),
            dma((2, 3, count)),
            dma((count,)),
            dma((2, count)),
            dma((2, count)),
            dma((2, count)),
        ],
        compiler_params=pltpu.CompilerParams(
            collective_id=0, has_side_effects=True, vmem_limit_bytes=VMEM_LIMIT
        ),
        name="mixer",
    )(
        conv_input,
        gate_input,
        conv_weight,
        conv_bias,
        x_weight.T,
        dt_gain[None, :],
        dt_weight,
        dt_bias[None, :],
        a_log,
        skip[None, :],
    )


def solution(mesh):
    return jax.shard_map(
        local,
        mesh=mesh,
        in_specs=(
            P(("batch", "seq"), None),
            P(("batch", "seq"), None),
            P(None, "seq"),
            P("seq"),
            P("seq", None),
            P(),
            P(None, "seq"),
            P("seq"),
            P(None, "seq"),
            P("seq"),
        ),
        out_specs=P(("batch", "seq"), None),
        check_vma=False,
    )
```
